32 devices in a mesh: lon: 16 (over z, x, core), lat: 2 (over y).
Axes of the slice: x: 2, y: 2, z: 4, core: 2. Of those that a mesh axis runs over, the one named last changes fastest.
Arguments:
- tokens: bfloat16 [2, 24, 73728], P(None, 'lat', 'lon'), may hold values from -6 to 6
- cotangent: bfloat16 [2, 12, 73728], P(None, 'lat', 'lon'), may hold values from -6 to 6
- kinds_one: int32 [1, 4], P(None, 'lat'), may hold values from 0 to 7
- kinds_two: int32 [1, 2], P(None, 'lat'), may hold values from 0 to 7
- table_one: float32 [8, 6, 3312], replicated, may hold values from -2 to 260
- table_two: float32 [8, 12, 3312], replicated, may hold values from -2 to 260
- gain_one: float32 [192], replicated, may hold values from 0.1 to 1.9
- gain_merge: float32 [768], replicated, may hold values from 0.1 to 1.9
- gain_two: float32 [384], replicated, may hold values from 0.1 to 1.9
- qkv_one: bfloat16 [192, 576], replicated, may hold values from -0.4375 to 0.4375
- proj_one: bfloat16 [192, 192], replicated, may hold values from -0.4375 to 0.4375
- merge_weight: bfloat16 [768, 384], replicated, may hold values from -0.21875 to 0.21875
- qkv_two: bfloat16 [384, 1152], replicated, may hold values from -0.3125 to 0.3125
- proj_two: bfloat16 [384, 384], replicated, may hold values from -0.3125 to 0.3125
Outputs:
- result: bfloat16 [2, 12, 73728], P(None, 'lat', 'lon')
- d_tokens: bfloat16 [2, 24, 73728], P(None, 'lat', 'lon')
- grad_qkv_one: bfloat16 [192, 576], replicated
- grad_proj_one: bfloat16 [192, 192], replicated
- grad_merge: bfloat16 [768, 384], replicated
- grad_qkv_two: bfloat16 [384, 1152], replicated
- grad_proj_two: bfloat16 [384, 384], replicated
The draws below stay inside these ranges and needn't reach their ends.
All inputs are finite; a program needn't handle non-finite values.
Results may differ from the reference program's by a relative error of at most 0.025.
Values may be sent and summed in bfloat16 or wider, within the bound.
No kernel may reach another device: no remote copies, remote signals or barrier semaphores. Data moves between devices by JAX's collectives and lax.ppermute only.
A program may use at most 128 MiB of HBM per device.

```python
import jax
import jax.numpy as jnp
import numpy as np
from jax import lax

C1 = 192
C2 = 384
HEADS1 = 6
HEADS2 = 12
WIN_Z = 2
WIN_LAT = 6
WIN_LON = 12
LEVELS = 2
TYPES = 8
RELS = 3312
H = 24
W = 384
H2 = 12
W2 = 192


def table_law(key, head_count, salt):
    own_key = jax.random.fold_in(key, salt)
    base_key = jax.random.fold_in(own_key, 11)
    values = jax.random.uniform(base_key, (TYPES, head_count, RELS), jnp.float32, -2.0, 2.0)
    return values


def draw_table_one(key, part):
    return table_law(key, HEADS1, 1)


def draw_table_two(key, part):
    return table_law(key, HEADS2, 2)


def with_ends(drawn, rng, low, largest):
    longest = drawn.shape.index(max(drawn.shape))
    spots = []
    for shift in (0, 1):
        where = [jax.random.randint(jax.random.fold_in(rng, axis), (), 0, length) for axis, length in enumerate(drawn.shape)]
        where[longest] = (where[longest] + shift) % drawn.shape[longest]
        spots.append(tuple(where))
    return drawn.at[spots[0]].set(low).at[spots[1]].set(largest)


def steps_of(stream_key, shape, split, smallest, top_value):
    def one(dim, shards_of):
        draws = jax.random.uniform(jax.random.fold_in(jax.random.fold_in(stream_key, 6), dim), (shards_of,), jnp.float32, smallest / len(split), top_value / len(split))
        return jnp.repeat(jnp.exp(draws), shape[dim] // shards_of).reshape((-1,) + (1,) * (len(shape) - dim - 1))

    level = one(*split[0])
    for cut in split[1:]:
        level = level * one(*cut)
    return level


def gaussian(rng, extent, scale, most, shards=(), held_as=jnp.bfloat16):
    values = jax.random.normal(rng, extent, jnp.float32) * scale
    if len(shards) > 0:
        values = steps_of(rng, extent, shards, -0.22, 0.18) * values
    return jnp.clip(values, min=-most, max=most).astype(held_as)


def setup_inputs(seed: int = 0) -> dict:
    arg_keys = jax.random.split(jax.random.key(seed), 15)
    return {
        "tokens": gaussian(arg_keys[0], (LEVELS, H, W * C1), 1.0, 6.0, ((1, 2), (2, 16))),
        "cotangent": gaussian(arg_keys[1], (LEVELS, H2, W2 * C2), 1.0, 6.0, ((1, 2), (2, 16))),
        "kinds_one": with_ends(jax.random.randint(arg_keys[2], (LEVELS // WIN_Z, H // WIN_LAT), 0, TYPES), jax.random.fold_in(arg_keys[2], 1), 0, TYPES - 1).astype(jnp.int32),
        "kinds_two": jax.random.randint(arg_keys[3], (LEVELS // WIN_Z, H2 // WIN_LAT), 0, TYPES).astype(jnp.int32),
        "table_one": draw_table_one(jax.random.fold_in(arg_keys[14], 71), 0),
        "table_two": draw_table_two(jax.random.fold_in(arg_keys[14], 71), 0),
        "gain_one": jnp.clip(1.0 + 0.18 * jax.random.normal(arg_keys[6], (C1,), jnp.float32), 0.1, 1.9),
        "gain_merge": jnp.clip(1.0 + 0.18 * jax.random.normal(arg_keys[7], (4 * C1,), jnp.float32), 0.1, 1.9),
        "gain_two": jnp.clip(1.0 + 0.18 * jax.random.normal(arg_keys[8], (C2,), jnp.float32), 0.1, 1.9),
        "qkv_one": gaussian(arg_keys[9], (C1, 3 * C1), C1 ** -0.5, 0.4375),
        "proj_one": gaussian(arg_keys[10], (C1, C1), C1 ** -0.5, 0.4375),
        "merge_weight": gaussian(arg_keys[11], (4 * C1, C2), (4 * C1) ** -0.5, 0.21875),
        "qkv_two": gaussian(arg_keys[12], (C2, 3 * C2), C2 ** -0.5, 0.3125),
        "proj_two": gaussian(arg_keys[13], (C2, C2), C2 ** -0.5, 0.3125),
    }


norm_epsilon = 1e-05
grad_epsilon = 1e-06
masked_score = -1e+30

def relative_table():
    window_size = WIN_Z * WIN_LAT * WIN_LON
    positions = np.arange(window_size)
    level_at = positions // (WIN_LAT * WIN_LON)
    row_at = positions // WIN_LON % WIN_LAT
    col_at = positions % WIN_LON
    joined = (level_at[:, None] * WIN_Z + level_at[None, :]) * (WIN_LAT * WIN_LAT)
    joined = joined + row_at[:, None] * WIN_LAT + row_at[None, :]
    joined = joined * (2 * WIN_LON - 1) + col_at[:, None] - col_at[None, :] + WIN_LON - 1
    return joined.astype(np.int32)

def layer_norm(values, scaling):
    centre = lax.optimization_barrier(jnp.mean(values, axis=-1, keepdims=True))
    spread = values - centre
    second = lax.optimization_barrier(jnp.mean(spread * spread, axis=-1, keepdims=True))
    return spread * lax.rsqrt(second + norm_epsilon) * scaling

def to_windows(lattice):
    level_count, row_count, col_count = lattice.shape[:3]
    trailing = lattice.shape[3:]
    trailing_axes = tuple(range(6, 6 + len(trailing)))
    pieces = lattice.reshape((level_count // WIN_Z, WIN_Z, row_count // WIN_LAT, WIN_LAT, col_count // WIN_LON, WIN_LON) + trailing)
    pieces = pieces.transpose((0, 2, 4, 1, 3, 5) + trailing_axes)
    return pieces.reshape((level_count // WIN_Z, row_count // WIN_LAT, col_count // WIN_LON, WIN_Z * WIN_LAT * WIN_LON) + trailing)

def from_windows(blocks, level_count, row_count, col_count):
    trailing = blocks.shape[4:]
    trailing_axes = tuple(range(6, 6 + len(trailing)))
    pieces = blocks.reshape((level_count // WIN_Z, row_count // WIN_LAT, col_count // WIN_LON, WIN_Z, WIN_LAT, WIN_LON) + trailing)
    pieces = pieces.transpose((0, 3, 1, 4, 2, 5) + trailing_axes)
    return pieces.reshape((level_count, row_count, col_count) + trailing)

def region_codes(level_count, row_start, row_count, rows_all):
    level_index = jnp.arange(level_count, dtype=jnp.int32)
    level_part = (level_index >= level_count - WIN_Z).astype(jnp.int32) + (level_index >= level_count - WIN_Z // 2).astype(jnp.int32)
    row_index = row_start + jnp.arange(row_count, dtype=jnp.int32)
    row_part = (row_index >= rows_all - WIN_LAT).astype(jnp.int32) + (row_index >= rows_all - WIN_LAT // 2).astype(jnp.int32)
    return level_part[:, None] * 3 + row_part[None, :]

def attend(shifted, kind_ids, bias_table, scaling, w_qkv, w_proj, head_count, row_start, rows_all, probe_qkv, probe_proj):
    level_count, row_count, col_count, channel_count = shifted.shape
    head_size = channel_count // head_count
    base_values = shifted.astype(jnp.float32)
    normed = layer_norm(base_values, scaling).astype(jnp.bfloat16)
    flat_rows = normed.reshape(-1, channel_count)
    packed = (jnp.dot(flat_rows, w_qkv, preferred_element_type=jnp.float32) + probe_qkv).astype(jnp.bfloat16)
    packed = to_windows(packed.reshape(level_count, row_count, col_count, 3, head_count, head_size))
    query_rows = packed[..., 0, :, :].astype(jnp.float32)
    key_rows = packed[..., 1, :, :].astype(jnp.float32)
    value_rows = packed[..., 2, :, :].astype(jnp.float32)
    scores = jnp.einsum('abdqhe,abdkhe->abdhqk', query_rows, key_rows) * head_size ** (-0.5)
    chosen = bias_table[kind_ids]
    full_bias = jnp.take(chosen, relative_table(), axis=3)
    scores = scores + full_bias[:, :, None]
    region_ids = region_codes(level_count, row_start, row_count, rows_all)
    tag_values = jnp.broadcast_to(region_ids[:, :, None], (level_count, row_count, col_count)).astype(jnp.float32)
    window_tags = to_windows(tag_values)
    allowed = window_tags[..., :, None] == window_tags[..., None, :]
    scores = jnp.where(allowed[:, :, :, None], scores, masked_score)
    row_top = lax.optimization_barrier(jnp.max(scores, axis=-1, keepdims=True))
    weights = jnp.exp(scores - row_top)
    attn_weights = (weights / lax.optimization_barrier(jnp.sum(weights, axis=-1, keepdims=True))).astype(jnp.bfloat16)
    attended = jnp.einsum('abdhqk,abdkhe->abdqhe', attn_weights.astype(jnp.float32), value_rows).astype(jnp.bfloat16)
    merged_rows = from_windows(attended, level_count, row_count, col_count).reshape(-1, channel_count)
    result = base_values.reshape(-1, channel_count) + jnp.dot(merged_rows, w_proj, preferred_element_type=jnp.float32) + probe_proj
    return (result.astype(jnp.bfloat16).reshape(shifted.shape), (flat_rows, merged_rows))

def merge_tokens(level_one, scaling, w_merge, probe_merge):
    level_count, row_count, col_count, channel_count = level_one.shape
    grouped = level_one.reshape(level_count, row_count // 2, 2, col_count // 2, 2, channel_count)
    grouped = grouped.transpose(0, 1, 3, 2, 4, 5).reshape(level_count, row_count // 2, col_count // 2, 4 * channel_count)
    normed = layer_norm(grouped.astype(jnp.float32), scaling).astype(jnp.bfloat16)
    flat_rows = normed.reshape(-1, 4 * channel_count)
    merged = (jnp.dot(flat_rows, w_merge, preferred_element_type=jnp.float32) + probe_merge).astype(jnp.bfloat16)
    return (merged.reshape(level_count, row_count // 2, col_count // 2, w_merge.shape[1]), flat_rows)

def weight_grad(inputs, cot_rows):
    return lax.dot_general(inputs, cot_rows.astype(jnp.bfloat16), (((0,), (0,)), ((), ())), preferred_element_type=jnp.float32)

def normalized(gradient):
    scale_back = lax.rsqrt(jnp.mean(gradient * gradient) + grad_epsilon)
    return (gradient * scale_back).astype(jnp.bfloat16)

def band_split(array, band_rows):
    level_count, row_count = array.shape[:2]
    band_stack = array.reshape((level_count, row_count // band_rows, band_rows) + array.shape[2:])
    return jnp.moveaxis(band_stack, 1, 0)

def band_join(band_stack):
    joined = jnp.moveaxis(band_stack, 0, 1)
    return joined.reshape((joined.shape[0], joined.shape[1] * joined.shape[2]) + joined.shape[3:])

def roll_ahead(lattice):
    return jnp.roll(lattice, (-(WIN_Z // 2), -(WIN_LAT // 2), -(WIN_LON // 2)), (0, 1, 2))

def roll_behind(lattice):
    return jnp.roll(lattice, (WIN_Z // 2, WIN_LAT // 2, WIN_LON // 2), (0, 1, 2))

def level_forward(shifted, kind_ids, bias_table, scaling, w_qkv, w_proj, head_count):
    rows_all = shifted.shape[1]
    band_count = rows_all // WIN_LAT
    operands = (band_split(shifted, WIN_LAT), band_split(kind_ids, 1), jnp.arange(band_count, dtype=jnp.int32) * WIN_LAT)

    def one_band(band_args):
        band_piece, kind_band, band_start = band_args
        token_count = band_piece.shape[0] * band_piece.shape[1] * band_piece.shape[2]
        channel_count = band_piece.shape[3]
        result, saved = attend(band_piece, kind_band, bias_table, scaling, w_qkv, w_proj, head_count, band_start, rows_all, jnp.zeros((token_count, 3 * channel_count), jnp.float32), jnp.zeros((token_count, channel_count), jnp.float32))
        return result
    return band_join(lax.map(one_band, operands))

def level_backward(shifted, kind_ids, bias_table, scaling, w_qkv, w_proj, head_count, cot_lattice):
    rows_all = shifted.shape[1]
    band_count = rows_all // WIN_LAT
    operands = (band_split(shifted, WIN_LAT), band_split(kind_ids, 1), jnp.arange(band_count, dtype=jnp.int32) * WIN_LAT, band_split(cot_lattice, WIN_LAT))

    def one_band(running, band_args):
        band_piece, kind_band, band_start, cot_band = band_args
        token_count = band_piece.shape[0] * band_piece.shape[1] * band_piece.shape[2]
        channel_count = band_piece.shape[3]

        def forward(lattice, probe_qkv, probe_proj):
            return attend(lattice, kind_band, bias_table, scaling, w_qkv, w_proj, head_count, band_start, rows_all, probe_qkv, probe_proj)
        result, pullback, saved = jax.vjp(forward, band_piece, jnp.zeros((token_count, 3 * channel_count), jnp.float32), jnp.zeros((token_count, channel_count), jnp.float32), has_aux=True)
        d_piece, d_packed, d_out = pullback(cot_band)
        running = (running[0] + weight_grad(saved[0], d_packed), running[1] + weight_grad(saved[1], d_out))
        return (running, d_piece)
    start_sums = (jnp.zeros(w_qkv.shape, jnp.float32), jnp.zeros(w_proj.shape, jnp.float32))
    sums, d_pieces = lax.scan(one_band, start_sums, operands)
    return (sums, band_join(d_pieces))

def merge_forward(level_one, scaling, w_merge):

    def one_band(band_piece):
        token_count = band_piece.shape[0] * (band_piece.shape[1] // 2) * (band_piece.shape[2] // 2)
        merged, flat_rows = merge_tokens(band_piece, scaling, w_merge, jnp.zeros((token_count, w_merge.shape[1]), jnp.float32))
        return merged
    return band_join(lax.map(one_band, band_split(level_one, 2 * WIN_LAT)))

def merge_backward(level_one, scaling, w_merge, cot_lattice):
    operands = (band_split(level_one, 2 * WIN_LAT), band_split(cot_lattice, WIN_LAT))

    def one_band(running, band_args):
        band_piece, cot_band = band_args
        token_count = band_piece.shape[0] * (band_piece.shape[1] // 2) * (band_piece.shape[2] // 2)

        def forward(lattice, probe_merge):
            return merge_tokens(lattice, scaling, w_merge, probe_merge)
        merged, pullback, flat_rows = jax.vjp(forward, band_piece, jnp.zeros((token_count, w_merge.shape[1]), jnp.float32), has_aux=True)
        d_piece, d_probe = pullback(cot_band)
        return (running + weight_grad(flat_rows, d_probe), d_piece)
    total, d_pieces = lax.scan(one_band, jnp.zeros(w_merge.shape, jnp.float32), operands)
    return (total, band_join(d_pieces))

def reference(tokens, cotangent, kinds_one, kinds_two, table_one, table_two, gain_one, gain_merge, gain_two, qkv_one, proj_one, merge_weight, qkv_two, proj_two):
    lattice = tokens.reshape(LEVELS, H, W, C1)
    shifted_one = roll_ahead(lattice)
    block_one = level_forward(shifted_one, kinds_one, table_one, gain_one, qkv_one, proj_one, HEADS1)
    level_one = roll_behind(block_one)
    merged = merge_forward(level_one, gain_merge, merge_weight)
    shifted_two = roll_ahead(merged)
    block_two = level_forward(shifted_two, kinds_two, table_two, gain_two, qkv_two, proj_two, HEADS2)
    level_two = roll_behind(block_two)
    d_block_two = roll_ahead(cotangent.reshape(LEVELS, H2, W2, C2))
    sums_two, d_shift_two = level_backward(shifted_two, kinds_two, table_two, gain_two, qkv_two, proj_two, HEADS2, d_block_two)
    d_merged = roll_behind(d_shift_two)
    raw_merge, d_level_one = merge_backward(level_one, gain_merge, merge_weight, d_merged)
    d_block_one = roll_ahead(d_level_one)
    sums_one, d_shift_one = level_backward(shifted_one, kinds_one, table_one, gain_one, qkv_one, proj_one, HEADS1, d_block_one)
    d_tokens = roll_behind(d_shift_one)
    return (level_two.reshape(LEVELS, H2, W2 * C2), d_tokens.reshape(LEVELS, H, W * C1), normalized(sums_one[0]), normalized(sums_one[1]), normalized(raw_merge), normalized(sums_two[0]), normalized(sums_two[1]))
```

```python
import functools

import jax
import jax.numpy as jnp
import numpy as np
from jax import lax
from jax.experimental import pallas as pl
from jax.experimental.pallas import tpu as pltpu
from jax.sharding import PartitionSpec as P

HEADS1 = 6
HEADS2 = 12
HEAD = 32
WIN_LAT = 6
WIN_LON = 12
HALF_LAT = WIN_LAT // 2
HALF_LON = WIN_LON // 2
SPOTS = WIN_LAT * WIN_LON
SPAN = 2 * WIN_LON - 1
LEVELS = 2

norm_epsilon = 1e-05
grad_epsilon = 1e-06
masked_score = -1e30

f32 = jnp.float32
bf16 = jnp.bfloat16
AXES = ("lon", "lat")


def rounded_up(count, step):
    return -(-count // step) * step


def mm(a, b):
    return lax.dot_general(a, b, (((1,), (0,)), ((), ())), preferred_element_type=f32)


def mm_nt(a, b):
    return lax.dot_general(a, b, (((1,), (1,)), ((), ())), preferred_element_type=f32)


def mm_tn(a, b):
    return lax.dot_general(a, b, (((0,), (0,)), ((), ())), preferred_element_type=f32)


def parts_rows(rows, cols, ahead):
    keep_r, keep_c = rows - HALF_LAT, cols - HALF_LON
    if ahead:
        row_sets = (range(HALF_LAT, rows), range(HALF_LAT))
        col_sets = (range(HALF_LON, cols), range(HALF_LON))
    else:
        row_sets = (range(keep_r), range(keep_r, rows))
        col_sets = (range(keep_c), range(keep_c, cols))
    out = []
    for rset, cset in ((0, 0), (1, 0), (0, 1), (1, 1)):
        piece = [(z, j, k) for z in range(LEVELS) for j in row_sets[rset] for k in col_sets[cset]]
        piece += [None] * (rounded_up(len(piece), 16) - len(piece))
        out.append(piece)
    return out


def window_rows(rows, cols):
    return [
        (z, b * WIN_LAT + ap, c * WIN_LON + bp)
        for b in range(rows // WIN_LAT)
        for c in range(cols // WIN_LON)
        for z in range(LEVELS)
        for ap in range(WIN_LAT)
        for bp in range(WIN_LON)
    ]


def merge_rows(rows, cols):
    return [
        (z, 2 * jj + a, 2 * kk + b)
        for a in range(2)
        for b in range(2)
        for z in range(LEVELS)
        for jj in range(rows // 2)
        for kk in range(cols // 2)
    ]


def lane_rows(rows, cols, pad):
    out = []
    for k in range(cols):
        group = [(1 - z, j, k) for j in range(rows) for z in range(LEVELS)]
        out += group + [None] * (pad - len(group))
    return out


def index_of(wanted, source):
    where = {spot: n for n, spot in enumerate(source) if spot is not None}
    return [-1 if spot is None else where[spot] for spot in wanted]


def flat(pieces):
    return [spot for piece in pieces for spot in piece]


def moved(pieces, dj, dk, rows, cols):
    return [
        None if s is None else (s[0], (s[1] + dj) % rows, (s[2] + dk) % cols) for s in flat(pieces)
    ]


def one_hot(index_ref, column, count, width):
    index = index_ref[0:count, column : column + 1]
    lanes = lax.broadcasted_iota(jnp.int32, (count, width), 1)
    return jnp.where(index == lanes, 1.0, 0.0).astype(bf16)


def lane_head_masks(width):
    lanes = lax.broadcasted_iota(jnp.int32, (1, width), 1)
    return [
        jnp.where((lanes >= h * HEAD) & (lanes < (h + 1) * HEAD), 1.0, 0.0).astype(f32)
        for h in range(width // HEAD)
    ]


def spread_heads(values, masks):
    return jnp.concatenate([values * m for m in masks], axis=0)


def gather_heads(stack, masks):
    total = stack[0:SPOTS] * masks[0]
    for h in range(1, len(masks)):
        total = total + stack[h * SPOTS : (h + 1) * SPOTS] * masks[h]
    return total


def head_groups(channels):
    out = []
    at = 0
    while at < channels:
        width = min(128, channels - at)
        out.append((at, width))
        at += width
    return out


def rms_stats(values):
    centre = jnp.mean(values, axis=-1, keepdims=True)
    spread = values - centre
    second = jnp.mean(spread * spread, axis=-1, keepdims=True)
    scale = lax.rsqrt(second + norm_epsilon)
    return spread * scale, scale


def norm_back(hat, scale, d_hat, count):
    first = jnp.sum(d_hat, axis=-1, keepdims=True) * (1.0 / count)
    second = jnp.sum(d_hat * hat, axis=-1, keepdims=True) * (1.0 / count)
    return scale * (d_hat - first - hat * second)


def softmax_rows(scores):
    top = jnp.max(scores, axis=-1, keepdims=True)
    weights = jnp.exp(scores - top)
    return weights / jnp.sum(weights, axis=-1, keepdims=True)


def bias_kernel(kinds_one, kinds_two, last, table_one, table_two, target, out_one, out_two, rows_ref, runs_ref):
    bands = out_one.shape[0] // LEVELS
    head_sets = [(8 * b, HEADS1) for b in range(bands)] + [(8 * bands, HEADS2)]
    width = WIN_LAT * SPAN
    slots = rows_ref.shape[0]
    rows_ref[...] = jnp.zeros(rows_ref.shape, f32)
    for b in range(bands):
        for h in range(HEADS1):
            rows_ref[8 * b + h : 8 * b + h + 1, :] = table_one[h, pl.ds(kinds_one[b], 1), :]
    for h in range(HEADS2):
        at = 8 * bands + h
        rows_ref[at : at + 1, :] = table_two[h, pl.ds(kinds_two[0], 1), :]
    runs_ref[...] = jnp.zeros(runs_ref.shape, f32)
    for z in range(LEVELS):
        for ap in range(WIN_LAT):
            start = (z * (LEVELS + 1)) * WIN_LAT * width + ap * width
            at = (z * WIN_LAT + ap) * slots
            runs_ref[at : at + slots, 0:width] = rows_ref[:, start : start + width]
    runs = runs_ref[...]
    high = runs.astype(bf16)
    rest = runs - high.astype(f32)
    middle = rest.astype(bf16)
    low = (rest - middle.astype(f32)).astype(bf16)
    sub = lax.broadcasted_iota(jnp.int32, (256, target.shape[1]), 0)
    pick = jnp.where(sub == target[0:1, :], 1.0, 0.0).astype(bf16)
    full = mm(high, pick) + mm(middle, pick) + mm(low, pick)
    lanes = lax.broadcasted_iota(jnp.int32, (1, 128), 1)
    for z in range(LEVELS):
        for ap in range(WIN_LAT):
            across = jnp.where(
                (lanes >= SPOTS // 2) if ap < HALF_LAT else (lanes < SPOTS // 2), masked_score, 0.0
            )
            at = (z * WIN_LAT + ap) * slots
            for s, (first, heads) in enumerate(head_sets):
                own = across * last[s].astype(f32)
                for bp in range(WIN_LON):
                    piece = full[at + first : at + first + heads, 128 * bp : 128 * bp + 128] + own
                    spot = ap * WIN_LON + bp
                    if s < bands:
                        out_one[s * LEVELS + z, pl.ds(spot, heads, stride=SPOTS), :] = piece
                    else:
                        out_two[z, pl.ds(spot, heads, stride=SPOTS), :] = piece


def expand_bias(kinds_one, kinds_two, last, table_one, table_two):
    bands = kinds_one.shape[0]
    target = np.full((8, WIN_LON * 128), -1, np.int32)
    for bp in range(WIN_LON):
        for aq in range(WIN_LAT):
            for bq in range(WIN_LON):
                target[:, bp * 128 + aq * WIN_LON + bq] = aq * SPAN + bp - bq + WIN_LON - 1
    slots = 8 * bands + rounded_up(HEADS2, 8)
    smem = pl.BlockSpec(memory_space=pltpu.SMEM)
    vmem = pl.BlockSpec(memory_space=pltpu.VMEM)
    return pl.pallas_call(
        bias_kernel,
        name="bias",
        in_specs=[smem, smem, smem, vmem, vmem, vmem],
        out_specs=[vmem, vmem],
        out_shape=(
            jax.ShapeDtypeStruct((bands * LEVELS, HEADS1 * SPOTS, 128), f32),
            jax.ShapeDtypeStruct((LEVELS, HEADS2 * SPOTS, 128), f32),
        ),
        scratch_shapes=[
            pltpu.VMEM((slots, table_one.shape[2]), f32),
            pltpu.VMEM((LEVELS * WIN_LAT * slots, 256), f32),
        ],
    )(kinds_one, kinds_two, last, table_one, table_two, target)


def unlace(main, lat, lon, diag, lace_ref, cut_row, cut_lane):
    rows = main.shape[0]
    lanes = main.shape[2]
    kept = lanes - cut_lane
    for j in range(rows - cut_row):
        lace_ref[2 * j : 2 * j + 2, 0:kept] = main[j + cut_row, :, cut_lane:lanes].astype(f32)
        lace_ref[2 * j : 2 * j + 2, kept:lanes] = lon[j].astype(f32)
    for n in range(cut_row):
        j = rows - cut_row + n
        lace_ref[2 * j : 2 * j + 2, 0:kept] = lat[n].astype(f32)
        lace_ref[2 * j : 2 * j + 2, kept:lanes] = diag[n].astype(f32)


def lace_out(lace_ref, main, lat, lon, diag, cut_row, cut_lane):
    rows = main.shape[0] + cut_row
    kept = main.shape[2]
    lanes = kept + cut_lane
    for j in range(rows - cut_row):
        main[j] = lace_ref[2 * j : 2 * j + 2, 0:kept].astype(bf16)
        lon[j] = lace_ref[2 * j : 2 * j + 2, kept:lanes].astype(bf16)
    for n in range(cut_row):
        j = rows - cut_row + n
        lat[n] = lace_ref[2 * j : 2 * j + 2, 0:kept].astype(bf16)
        diag[n] = lace_ref[2 * j : 2 * j + 2, kept:lanes].astype(bf16)


def forward_one_kernel(
    main, lat, lon, diag, bias, gain, w_qkv, w_proj, index,
    out_main, out_lat, out_lon, out_diag, keep_x, keep_packed, keep_probs, keep_att,
    lace_ref, packed_ref, att_ref,
    *, cols, columns,
):
    channels = gain.shape[1]
    lace_rows = lace_ref.shape[0]
    count = lace_rows * cols
    unlace(main, lat, lon, diag, lace_ref, HALF_LAT, HALF_LON * channels)
    stacked = jnp.concatenate(
        [lace_ref[:, channels * k : channels * (k + 1)] for k in range(cols)], axis=0
    ).astype(bf16)
    values = mm(one_hot(index, columns[0], count, count), stacked)
    hat, _ = rms_stats(values)
    normed = (hat * gain[0:1, :]).astype(bf16)
    packed = mm(normed, w_qkv[...]).astype(bf16)
    packed_ref[...] = packed.astype(f32)
    keep_packed[...] = packed
    keep_x[...] = values.astype(bf16)
    units = count // SPOTS
    bands_span = bias.shape[0] // LEVELS
    per_band = units // bands_span
    for u in range(units):
        band, level = u // per_band, u % LEVELS
        r0 = u * SPOTS
        for at, width in head_groups(channels):
            masks = lane_head_masks(width)
            h0 = at // HEAD
            query = packed_ref[r0 : r0 + SPOTS, at : at + width]
            key = packed_ref[r0 : r0 + SPOTS, channels + at : channels + at + width].astype(bf16)
            value = packed_ref[r0 : r0 + SPOTS, 2 * channels + at : 2 * channels + at + width].astype(bf16)
            rows = slice(h0 * SPOTS, (h0 + len(masks)) * SPOTS)
            scores = mm_nt(spread_heads(query, masks).astype(bf16), key) * HEAD ** (-0.5)
            scores = scores + bias[band * LEVELS + level, rows, 0:SPOTS]
            probs = softmax_rows(scores).astype(bf16)
            keep_probs[u, rows, 0:SPOTS] = probs
            att_ref[r0 : r0 + SPOTS, at : at + width] = gather_heads(mm(probs, value), masks)
    attended = att_ref[...].astype(bf16)
    keep_att[...] = attended
    block = (values + mm(attended, w_proj[...])).astype(bf16)
    start = 0
    total = out_main.shape[0] + out_lat.shape[0] + out_lon.shape[0] + out_diag.shape[0]
    parts = mm(one_hot(index, columns[1], total, count), block).astype(bf16)
    for out in (out_main, out_lat, out_lon, out_diag):
        out[...] = parts[start : start + out.shape[0]]
        start += out.shape[0]


def merge_two_kernel(
    core, main, lat, lon, diag, cot_main, cot_lat, cot_lon, cot_diag, bias,
    gain_merge, gain_two, w_merge, w_qkv, w_proj, index,
    res_main, res_lat, res_lon, res_diag, d_main, d_lat, d_lon, d_diag, sums_keep, sums_send,
    lace_ref, probs_ref, packed_ref, att_ref, d_packed_ref, sums_ref,
    *, cols, columns,
):
    channels = gain_two.shape[1]
    thin = main.shape[1]
    groups = gain_merge.shape[1] // thin
    tokens = LEVELS * SPOTS
    total = main.shape[0] + lat.shape[0] + lon.shape[0] + diag.shape[0]
    stacked = jnp.concatenate([main[...], lat[...], lon[...], diag[...]], axis=0)
    grouped = mm(one_hot(index, columns[0], groups * tokens, total), stacked)
    pieces = [grouped[g * tokens : (g + 1) * tokens] for g in range(groups)]
    wide = groups * thin
    centre = sum(jnp.sum(p, axis=-1, keepdims=True) for p in pieces) * (1.0 / wide)
    spreads = [p - centre for p in pieces]
    second = sum(jnp.sum(s * s, axis=-1, keepdims=True) for s in spreads) * (1.0 / wide)
    scale_merge = lax.rsqrt(second + norm_epsilon)
    hats = [s * scale_merge for s in spreads]
    gains = [gain_merge[0:1, g * thin : (g + 1) * thin] for g in range(groups)]
    merged_norm = [(hats[g] * gains[g]).astype(bf16) for g in range(groups)]
    merged = mm(merged_norm[0], w_merge[0:thin, :])
    for g in range(1, groups):
        merged = merged + mm(merged_norm[g], w_merge[g * thin : (g + 1) * thin, :])
    merged = merged.astype(bf16).astype(f32)
    hat, scale_two = rms_stats(merged)
    normed = (hat * gain_two[0:1, :]).astype(bf16)
    packed_ref[...] = mm(normed, w_qkv[...]).astype(bf16).astype(f32)
    masks = lane_head_masks(128)
    per = len(masks)
    for z in range(LEVELS):
        r0 = z * SPOTS
        for at, width in head_groups(channels):
            h0 = at // HEAD
            rows = slice(h0 * SPOTS, (h0 + per) * SPOTS)
            query = packed_ref[r0 : r0 + SPOTS, at : at + width]
            key = packed_ref[r0 : r0 + SPOTS, channels + at : channels + at + width].astype(bf16)
            value = packed_ref[r0 : r0 + SPOTS, 2 * channels + at : 2 * channels + at + width].astype(bf16)
            scores = mm_nt(spread_heads(query, masks).astype(bf16), key) * HEAD ** (-0.5)
            probs = softmax_rows(scores + bias[z, rows, 0:SPOTS])
            probs_ref[z, rows, 0:SPOTS] = probs
            att_ref[r0 : r0 + SPOTS, at : at + width] = gather_heads(mm(probs.astype(bf16), value), masks)
    attended = att_ref[...].astype(bf16)
    block = (merged + mm(attended, w_proj[...])).astype(bf16)
    lace_rows = lace_ref.shape[0]
    lattice = mm(one_hot(index, columns[1], lace_rows * cols, tokens), block)
    for k in range(cols):
        lace_ref[:, channels * k : channels * (k + 1)] = lattice[lace_rows * k : lace_rows * (k + 1)]
    lace_out(lace_ref, res_main, res_lat, res_lon, res_diag, HALF_LAT, HALF_LON * channels)
    lace_ref[...] = jnp.zeros(lace_ref.shape, f32)
    unlace(cot_main, cot_lat, cot_lon, cot_diag, lace_ref, HALF_LAT, HALF_LON * channels)
    cot_stack = jnp.concatenate(
        [lace_ref[:, channels * k : channels * (k + 1)] for k in range(cols)], axis=0
    ).astype(bf16)
    d_block = mm(one_hot(index, columns[2], tokens, lace_rows * cols), cot_stack)
    d_block_low = d_block.astype(bf16)
    at_sum = groups * thin
    sums_ref[at_sum : at_sum + channels, :] = mm_tn(attended, d_block_low)
    att_ref[...] = mm_nt(d_block_low, w_proj[...]).astype(bf16).astype(f32)
    for z in range(LEVELS):
        r0 = z * SPOTS
        for at, width in head_groups(channels):
            h0 = at // HEAD
            rows = slice(h0 * SPOTS, (h0 + per) * SPOTS)
            attention_back(
                packed_ref, att_ref, d_packed_ref, probs_ref[z, rows, 0:SPOTS], masks, r0, at, width, channels
            )
    d_packed = d_packed_ref[...].astype(bf16)
    at_sum += channels
    for n in range(3):
        sums_ref[at_sum + n * channels : at_sum + (n + 1) * channels, :] = mm_tn(
            normed, d_packed[:, n * channels : (n + 1) * channels]
        )
    d_normed = mm_nt(d_packed, w_qkv[...]).astype(bf16).astype(f32)
    d_merged = d_block + norm_back(hat, scale_two, d_normed * gain_two[0:1, :], channels)
    d_merged = d_merged.astype(bf16)
    d_hats = []
    for g in range(groups):
        sums_ref[g * thin : (g + 1) * thin, :] = mm_tn(merged_norm[g], d_merged)
        d_norm = mm_nt(d_merged, w_merge[g * thin : (g + 1) * thin, :]).astype(bf16).astype(f32)
        d_hats.append(d_norm * gains[g])
    first = sum(jnp.sum(d, axis=-1, keepdims=True) for d in d_hats) * (1.0 / wide)
    cross = sum(jnp.sum(d * h, axis=-1, keepdims=True) for d, h in zip(d_hats, hats)) * (1.0 / wide)
    d_group = jnp.concatenate(
        [scale_merge * (d_hats[g] - first - hats[g] * cross) for g in range(groups)], axis=0
    ).astype(bf16)
    parts = mm(one_hot(index, columns[3], total, groups * tokens), d_group).astype(bf16)
    start = 0
    for out in (d_main, d_lat, d_lon, d_diag):
        out[...] = parts[start : start + out.shape[0]]
        start += out.shape[0]
    half = sums_ref.shape[0] // 2
    mine = core[0]
    first_row = pl.multiple_of(mine * half, 16)
    other_row = pl.multiple_of((1 - mine) * half, 16)
    sums_keep[...] = sums_ref[pl.ds(first_row, half), :].astype(bf16)
    sums_send[...] = sums_ref[pl.ds(other_row, half), :].astype(bf16)


def attention_back(packed_ref, d_att_ref, d_packed_ref, probs, masks, r0, at, width, channels):
    query = packed_ref[r0 : r0 + SPOTS, at : at + width]
    key = packed_ref[r0 : r0 + SPOTS, channels + at : channels + at + width].astype(bf16)
    value = packed_ref[r0 : r0 + SPOTS, 2 * channels + at : 2 * channels + at + width].astype(bf16)
    d_att = spread_heads(d_att_ref[r0 : r0 + SPOTS, at : at + width], masks).astype(bf16)
    probs_low = probs.astype(bf16)
    probs = probs.astype(f32)
    d_probs = mm_nt(d_att, value).astype(bf16).astype(f32)
    d_value = mm_tn(probs_low, d_att)
    inner = jnp.sum(probs * d_probs, axis=-1, keepdims=True)
    d_scores = (probs * (d_probs - inner) * HEAD ** (-0.5)).astype(bf16)
    d_query = gather_heads(mm(d_scores, key), masks)
    d_key = mm_tn(d_scores, spread_heads(query, masks).astype(bf16))
    d_packed_ref[r0 : r0 + SPOTS, at : at + width] = d_query
    d_packed_ref[r0 : r0 + SPOTS, channels + at : channels + at + width] = d_key
    d_packed_ref[r0 : r0 + SPOTS, 2 * channels + at : 2 * channels + at + width] = d_value


def backward_one_kernel(
    core, main, lat, lon, diag, keep_x, keep_packed, keep_probs, keep_att, gain, w_qkv, w_proj, index,
    out_main, out_lat, out_lon, out_diag, sums_keep, sums_send,
    lace_ref, packed_ref, att_ref, d_packed_ref, sums_ref,
    *, cols, columns,
):
    channels = gain.shape[1]
    lace_rows = lace_ref.shape[0]
    count = lace_rows * cols
    total = main.shape[0] + lat.shape[0] + lon.shape[0] + diag.shape[0]
    stacked = jnp.concatenate([main[...], lat[...], lon[...], diag[...]], axis=0)
    d_block = mm(one_hot(index, columns[0], count, total), stacked)
    d_block_low = d_block.astype(bf16)
    hat, scale = rms_stats(keep_x[...].astype(f32))
    normed = (hat * gain[0:1, :]).astype(bf16)
    packed_ref[...] = keep_packed[...].astype(f32)
    att_ref[...] = mm_nt(d_block_low, w_proj[...]).astype(bf16).astype(f32)
    for u in range(count // SPOTS):
        r0 = u * SPOTS
        for at, width in head_groups(channels):
            masks = lane_head_masks(width)
            h0 = at // HEAD
            rows = slice(h0 * SPOTS, (h0 + len(masks)) * SPOTS)
            attention_back(
                packed_ref, att_ref, d_packed_ref, keep_probs[u, rows, 0:SPOTS], masks, r0, at, width, channels
            )
    d_packed = d_packed_ref[...].astype(bf16)
    sums_ref[:, 0 : 3 * channels] = mm_tn(normed, d_packed)
    sums_ref[:, 3 * channels : 4 * channels] = mm_tn(keep_att[...], d_block_low)
    d_normed = mm_nt(d_packed, w_qkv[...]).astype(bf16).astype(f32)
    d_shift = d_block + norm_back(hat, scale, d_normed * gain[0:1, :], channels)
    lattice = mm(one_hot(index, columns[1], count, count), d_shift.astype(bf16))
    for k in range(cols):
        lace_ref[:, channels * k : channels * (k + 1)] = lattice[lace_rows * k : lace_rows * (k + 1)]
    lace_out(lace_ref, out_main, out_lat, out_lon, out_diag, HALF_LAT, HALF_LON * channels)
    mine = core[0]
    half = 2 * channels
    low = sums_ref[:, 0:half].astype(bf16)
    high = sums_ref[:, half : 2 * half].astype(bf16)

    @pl.when(mine == 0)
    def _():
        sums_keep[...] = low
        sums_send[...] = high

    @pl.when(mine != 0)
    def _():
        sums_keep[...] = high
        sums_send[...] = low


def sizes():
    return lax.axis_size("lon"), lax.axis_size("lat")


def send(values, lon_step, lat_step):
    nlon, nlat = sizes()
    route = [
        (i * nlat + j, ((i + lon_step) % nlon) * nlat + (j + lat_step) % nlat)
        for i in range(nlon)
        for j in range(nlat)
    ]
    return lax.ppermute(values, AXES, route)


def exchange(lat, lon, diag, step):
    return send(lat, 0, step), send(lon, step, 0), send(diag, step, step)


def halos(lattice, cut_row, cut_lane):
    return (
        lattice[:cut_row, :, cut_lane:],
        lattice[cut_row:, :, :cut_lane],
        lattice[:cut_row, :, :cut_lane],
    )


def joined(main, lat, lon, diag):
    top = jnp.concatenate([diag, lat], axis=2)
    rest = jnp.concatenate([lon, main], axis=2)
    return jnp.concatenate([top, rest], axis=0).transpose(1, 0, 2)


def place_stages():
    nlon, nlat = sizes()
    near_lon = 2 if nlon % 4 == 0 else 1
    near_lat = 2 if nlat % 2 == 0 else 1
    far_lon = nlon // 2 // near_lon
    far_lat = nlat // near_lat

    def near(i, j, d):
        c, x, z = i % 2, i // 2 % near_lon, i // 2 // near_lon
        y, w = j % near_lat, j // near_lat
        place = (x * near_lat + y) ^ d
        return (z * near_lon + place // near_lat) * 2 + c, w * near_lat + place % near_lat

    def wide(i, j, d):
        z = i // 2 // near_lon
        return ((z + d) % far_lon) * 2 * near_lon + i % (2 * near_lon), j

    def high(i, j, d):
        return i, ((j // near_lat + d) % far_lat) * near_lat + j % near_lat

    lon_at, lat_at = lax.axis_index("lon"), lax.axis_index("lat")
    near_at = (lon_at // 2 % near_lon) * near_lat + lat_at % near_lat
    stages = [
        (near_lon * near_lat, near, near_at, lambda at, d: at ^ d, lambda at, d: at ^ d),
        (far_lon, wide, lon_at // 2 // near_lon, lambda at, d: (at + d) % far_lon, lambda at, d: (at - d) % far_lon),
        (far_lat, high, lat_at // near_lat, lambda at, d: (at + d) % far_lat, lambda at, d: (at - d) % far_lat),
    ]
    return [s for s in stages if s[0] > 1]


def hop(values, step, d):
    nlon, nlat = sizes()
    route = []
    for i in range(nlon):
        for j in range(nlat):
            to_lon, to_lat = step(i, j, d)
            route.append((i * nlat + j, to_lon * nlat + to_lat))
    return lax.ppermute(values, AXES, route)


def pair(values):
    nlon, nlat = sizes()
    route = [(i * nlat + j, (i ^ 1) * nlat + j) for i in range(nlon) for j in range(nlat)]
    return lax.ppermute(values, AXES, route)


def reduce_stages(keep, sent):
    value = (keep.astype(f32) + pair(sent).astype(f32)).astype(bf16)
    taken = []
    for size, step, at, target, source in place_stages():
        rows = value.shape[0]
        split = rows % size == 0
        taken.append((size, step, at, source, split))
        if split:
            chunks = value.reshape(size, rows // size, value.shape[1])
            total = lax.dynamic_index_in_dim(chunks, at, 0, False).astype(f32)
            got = [
                hop(lax.dynamic_index_in_dim(chunks, target(at, d), 0, False), step, d)
                for d in range(1, size)
            ]
        else:
            total = value.astype(f32)
            got = [hop(value, step, d) for d in range(1, size)]
        for part in got:
            total = total + part.astype(f32)
        value = total.astype(bf16)
    return value, taken


def gather_stages(value, taken):
    pieces = value[None]
    places = [jnp.int32(0)]
    span = 1
    for size, step, at, source, split in reversed(taken):
        if not split:
            continue
        got = [pieces] + [hop(pieces, step, d) for d in range(1, size)]
        pieces = jnp.concatenate(got, axis=0)
        places = [source(at, d).astype(jnp.int32) * span + p for d in range(size) for p in places]
        span *= size
    return pieces, pair(pieces), jnp.stack(places)


def finish_kernel(core, place_two, place_one, own_two, far_two, own_one, far_one,
                  g_qkv_one, g_proj_one, g_merge, g_qkv_two, g_proj_two, two_ref, one_ref):
    mine = core[0]
    count = own_two.shape[0]
    for n in range(count):
        at = place_two[n]
        two_ref[mine * count + at] = own_two[n].astype(f32)
        two_ref[(1 - mine) * count + at] = far_two[n].astype(f32)
    count = own_one.shape[0]
    for n in range(count):
        at = place_one[n]
        one_ref[mine * count + at] = own_one[n].astype(f32)
        one_ref[(1 - mine) * count + at] = far_one[n].astype(f32)

    def scale_of(parts, entries):
        total = parts[0]
        for p in parts[1:]:
            total = total + p
        return lax.rsqrt(jnp.sum(total, axis=0, keepdims=True).sum(axis=1, keepdims=True) * (1.0 / entries) + grad_epsilon)

    def spans(ref, first, last):
        rows = ref.shape[1]
        while first < last:
            n, inside = first // rows, first % rows
            size = min(rows - inside, last - first)
            yield n, inside, size, first
            first += size

    def squares(ref, first, last, lanes):
        return [
            jnp.sum(jnp.square(ref[n, i : i + s, lanes]), axis=0, keepdims=True)
            for n, i, s, _ in spans(ref, first, last)
        ]

    channels = g_proj_two.shape[0]
    wide = g_merge.shape[0]
    every = slice(0, channels)
    jobs = (
        (g_merge, [(0, wide, 0)]),
        (g_proj_two, [(wide, wide + channels, 0)]),
        (g_qkv_two, [(wide + (n + 1) * channels, wide + (n + 2) * channels, n * channels) for n in range(3)]),
    )
    for out, blocks in jobs:
        parts = [q for first, last, _ in blocks for q in squares(two_ref, first, last, every)]
        scale = scale_of(parts, out.shape[0] * out.shape[1])
        for first, last, lane in blocks:
            for n, i, s, row in spans(two_ref, first, last):
                r = row - first
                out[r : r + s, lane : lane + channels] = (two_ref[n, i : i + s, :] * scale).astype(bf16)
    thin = g_proj_one.shape[0]
    first_half = squares(one_ref, 0, thin, slice(0, 2 * thin))
    second = squares(one_ref, thin, 2 * thin, slice(0, 2 * thin))
    lanes = lax.broadcasted_iota(jnp.int32, (1, 2 * thin), 1)
    qkv_parts = first_half + [jnp.where(lanes < thin, p, 0.0) for p in second]
    proj_parts = [jnp.where(lanes < thin, 0.0, p) for p in second]
    scale_qkv = scale_of(qkv_parts, 3 * thin * thin)
    scale_proj = scale_of(proj_parts, thin * thin)
    for n, i, s, row in spans(one_ref, 0, thin):
        g_qkv_one[row : row + s, 0 : 2 * thin] = (one_ref[n, i : i + s, :] * scale_qkv).astype(bf16)
    for n, i, s, row in spans(one_ref, thin, 2 * thin):
        r = row - thin
        g_qkv_one[r : r + s, 2 * thin : 3 * thin] = (one_ref[n, i : i + s, 0:thin] * scale_qkv).astype(bf16)
        g_proj_one[r : r + s, :] = (one_ref[n, i : i + s, thin : 2 * thin] * scale_proj).astype(bf16)


def shards(
    tokens, cotangent, kinds_one, kinds_two, table_one, table_two, gain_one, gain_merge, gain_two,
    qkv_one, proj_one, merge_weight, qkv_two, proj_two,
):
    c1, c2 = proj_one.shape[0], proj_two.shape[0]
    rows1, cols1 = tokens.shape[1], tokens.shape[2] // c1
    rows2, cols2 = rows1 // 2, cols1 // 2
    bands = rows1 // WIN_LAT
    nlon, nlat = sizes()
    smem = pl.BlockSpec(memory_space=pltpu.SMEM)
    vmem = pl.BlockSpec(memory_space=pltpu.VMEM)
    core = (lax.axis_index("lon") % 2).astype(jnp.int32)[None]
    at_end = (lax.axis_index("lat") == nlat - 1).astype(jnp.int32)
    last = jnp.stack([jnp.int32(0)] * (bands - 1) + [at_end, at_end])

    lace1 = lane_rows(rows1, cols1, LEVELS * rows1)
    lace2_pad = rounded_up(LEVELS * rows2, 8)
    lace2 = lane_rows(rows2, cols2, lace2_pad)
    win1, win2 = window_rows(rows1, cols1), window_rows(rows2, cols2)
    group = merge_rows(rows1, cols1)
    ahead = parts_rows(rows1, cols1, True)
    behind = parts_rows(rows1, cols1, False)
    ahead_got = moved(ahead, -HALF_LAT, -HALF_LON, rows1, cols1)
    behind_got = moved(behind, HALF_LAT, HALF_LON, rows1, cols1)
    orders = [
        index_of(win1, lace1),
        index_of(flat(ahead), win1),
        index_of(group, ahead_got),
        index_of(lace2, win2),
        index_of(win2, lace2),
        index_of(flat(behind), group),
        index_of(win1, behind_got),
        index_of(lace1, win1),
    ]
    index = np.full((max(len(o) for o in orders), 128), -1, np.int32)
    for n, order in enumerate(orders):
        index[: len(order), n] = order
    index = jnp.asarray(index)
    sizes_parts = [len(p) for p in ahead]

    lattice = tokens.transpose(1, 0, 2)
    cot = cotangent.transpose(1, 0, 2)
    lane1, lane2 = HALF_LON * c1, HALF_LON * c2
    tok_halos = exchange(*halos(lattice, HALF_LAT, lane1), -1)
    bias_one, bias_two = expand_bias(
        kinds_one[0], kinds_two[0], last, table_one.swapaxes(0, 1), table_two.swapaxes(0, 1)
    )
    cot_halos = exchange(*halos(cot, HALF_LAT, lane2), -1)

    def part_shapes(dtype=bf16):
        return [jax.ShapeDtypeStruct((n, c1), dtype) for n in sizes_parts]

    def lace_shapes(rows, cols, channels):
        kr, kl, cl = rows - HALF_LAT, (cols - HALF_LON) * channels, HALF_LON * channels
        return [
            jax.ShapeDtypeStruct((r, LEVELS, n), bf16)
            for r, n in ((kr, kl), (HALF_LAT, kl), (kr, cl), (HALF_LAT, cl))
        ]

    count1 = LEVELS * rows1 * cols1
    units1 = count1 // SPOTS
    fwd = pl.pallas_call(
        functools.partial(forward_one_kernel, cols=cols1, columns=(0, 1)),
        name="forward_one",
        in_specs=[vmem] * 9,
        out_specs=[vmem] * 8,
        out_shape=part_shapes()
        + [
            jax.ShapeDtypeStruct((count1, c1), bf16),
            jax.ShapeDtypeStruct((count1, 3 * c1), bf16),
            jax.ShapeDtypeStruct((units1, HEADS1 * SPOTS, 128), bf16),
            jax.ShapeDtypeStruct((count1, c1), bf16),
        ],
        scratch_shapes=[
            pltpu.VMEM((LEVELS * rows1, cols1 * c1), f32),
            pltpu.VMEM((count1, 3 * c1), f32),
            pltpu.VMEM((count1, c1), f32),
        ],
    )(lattice, *tok_halos, bias_one, gain_one[None], qkv_one, proj_one, index)
    parts, kept = fwd[:4], fwd[4:]
    got = exchange(*parts[1:], -1)

    tokens2 = LEVELS * SPOTS
    total_two = 4 * c1 + 4 * c2
    two = pl.pallas_call(
        functools.partial(merge_two_kernel, cols=cols2, columns=(2, 3, 4, 5)),
        name="merge_two",
        in_specs=[smem] + [vmem] * 15,
        out_specs=[vmem] * 10,
        out_shape=lace_shapes(rows2, cols2, c2)
        + part_shapes()
        + [jax.ShapeDtypeStruct((total_two // 2, c2), bf16)] * 2,
        scratch_shapes=[
            pltpu.VMEM((lace2_pad, cols2 * c2), f32),
            pltpu.VMEM((LEVELS, HEADS2 * SPOTS, 128), f32),
            pltpu.VMEM((tokens2, 3 * c2), f32),
            pltpu.VMEM((tokens2, c2), f32),
            pltpu.VMEM((tokens2, 3 * c2), f32),
            pltpu.VMEM((total_two, c2), f32),
        ],
    )(core, parts[0], *got, cot, *cot_halos, bias_two, gain_merge[None], gain_two[None],
      merge_weight, qkv_two, proj_two, index)
    res, d_parts, sums_two = two[:4], two[4:8], two[8:]
    d_got = exchange(*d_parts[1:], 1)
    value_two, taken_two = reduce_stages(*sums_two)

    one = pl.pallas_call(
        functools.partial(backward_one_kernel, cols=cols1, columns=(6, 7)),
        name="backward_one",
        in_specs=[smem] + [vmem] * 12,
        out_specs=[vmem] * 6,
        out_shape=lace_shapes(rows1, cols1, c1) + [jax.ShapeDtypeStruct((c1, 2 * c1), bf16)] * 2,
        scratch_shapes=[
            pltpu.VMEM((LEVELS * rows1, cols1 * c1), f32),
            pltpu.VMEM((count1, 3 * c1), f32),
            pltpu.VMEM((count1, c1), f32),
            pltpu.VMEM((count1, 3 * c1), f32),
            pltpu.VMEM((c1, 4 * c1), f32),
        ],
    )(core, d_parts[0], *d_got, *kept, gain_one[None], qkv_one, proj_one, index)
    d_tok, sums_one = one[:4], one[4:]
    value_one, taken_one = reduce_stages(*sums_one)
    result = joined(res[0], *exchange(*res[1:], 1))
    d_tokens = joined(d_tok[0], *exchange(*d_tok[1:], 1))

    own_two, far_two, place_two = gather_stages(value_two, taken_two)
    own_one, far_one, place_one = gather_stages(value_one, taken_one)
    grads = pl.pallas_call(
        finish_kernel,
        name="finish",
        in_specs=[smem] * 3 + [vmem] * 4,
        out_specs=[vmem] * 5,
        out_shape=[
            jax.ShapeDtypeStruct(w.shape, bf16) for w in (qkv_one, proj_one, merge_weight, qkv_two, proj_two)
        ],
        scratch_shapes=[
            pltpu.VMEM((2 * own_two.shape[0],) + own_two.shape[1:], f32),
            pltpu.VMEM((2 * own_one.shape[0],) + own_one.shape[1:], f32),
        ],
    )(core, place_two, place_one, own_two, far_two, own_one, far_one)
    return (result, d_tokens, *grads)


def solution(mesh):
    tiled = P(None, "lat", "lon")
    in_specs = (tiled, tiled, P(None, "lat"), P(None, "lat")) + (P(),) * 10
    out_specs = (tiled, tiled, P(), P(), P(), P(), P())
    return jax.shard_map(shards, mesh=mesh, in_specs=in_specs, out_specs=out_specs, check_vma=False)
```

```python
import functools

import jax
import jax.numpy as jnp
import numpy as np
from jax import lax
from jax.experimental import pallas as pl
from jax.experimental.pallas import tpu as pltpu
from jax.sharding import PartitionSpec as P


HEADS1 = 6
HEADS2 = 12
HEAD = 32
WIN_LAT = 6
WIN_LON = 12
HALF_LAT = WIN_LAT // 2
HALF_LON = WIN_LON // 2
SPOTS = WIN_LAT * WIN_LON
SPAN = 2 * WIN_LON - 1
LEVELS = 2

norm_epsilon = 1e-05
grad_epsilon = 1e-06
masked_score = -1e30

f32 = jnp.float32
bf16 = jnp.bfloat16
AXES = ("lon", "lat")


def rounded_up(count, step):
    return -(-count // step) * step


def core_of():
    return lax.axis_index("lon") % 2


def mm(a, b):
    return lax.dot_general(a, b, (((1,), (0,)), ((), ())), preferred_element_type=f32)


def mm_nt(a, b):
    return lax.dot_general(a, b, (((1,), (1,)), ((), ())), preferred_element_type=f32)


def mm_tn(a, b):
    return lax.dot_general(a, b, (((0,), (0,)), ((), ())), preferred_element_type=f32)


def parts_rows(rows, cols, ahead):
    keep_r, keep_c = rows - HALF_LAT, cols - HALF_LON
    if ahead:
        row_sets = (range(HALF_LAT, rows), range(HALF_LAT))
        col_sets = (range(HALF_LON, cols), range(HALF_LON))
    else:
        row_sets = (range(keep_r), range(keep_r, rows))
        col_sets = (range(keep_c), range(keep_c, cols))
    out = []
    for rset, cset in ((0, 0), (1, 0), (0, 1), (1, 1)):
        piece = [(z, j, k) for z in range(LEVELS) for j in row_sets[rset] for k in col_sets[cset]]
        piece += [None] * (rounded_up(len(piece), 16) - len(piece))
        out.append(piece)
    return out


def window_rows(rows, cols):
    return [
        (z, b * WIN_LAT + ap, c * WIN_LON + bp)
        for b in range(rows // WIN_LAT)
        for c in range(cols // WIN_LON)
        for z in range(LEVELS)
        for ap in range(WIN_LAT)
        for bp in range(WIN_LON)
    ]


def merge_rows(rows, cols):
    return [
        (z, 2 * jj + a, 2 * kk + b)
        for a in range(2)
        for b in range(2)
        for z in range(LEVELS)
        for jj in range(rows // 2)
        for kk in range(cols // 2)
    ]


def lane_rows(rows, cols, pad):
    out = []
    for k in range(cols):
        group = [(1 - z, j, k) for j in range(rows) for z in range(LEVELS)]
        out += group + [None] * (pad - len(group))
    return out


def index_of(wanted, source):
    where = {spot: n for n, spot in enumerate(source) if spot is not None}
    return [-1 if spot is None else where[spot] for spot in wanted]


def flat(pieces):
    return [spot for piece in pieces for spot in piece]


def moved(pieces, dj, dk, rows, cols):
    return [
        None if s is None else (s[0], (s[1] + dj) % rows, (s[2] + dk) % cols) for s in flat(pieces)
    ]


def one_hot(index_ref, column, count, width):
    index = index_ref[0:count, column : column + 1]
    lanes = lax.broadcasted_iota(jnp.int32, (count, width), 1)
    return jnp.where(index == lanes, 1.0, 0.0).astype(bf16)


def lane_head_masks(width):
    lanes = lax.broadcasted_iota(jnp.int32, (1, width), 1)
    return [
        jnp.where((lanes >= h * HEAD) & (lanes < (h + 1) * HEAD), 1.0, 0.0).astype(f32)
        for h in range(width // HEAD)
    ]


def spread_heads(values, masks):
    return jnp.concatenate([values * m for m in masks], axis=0)


def gather_heads(stack, masks):
    total = stack[0:SPOTS] * masks[0]
    for h in range(1, len(masks)):
        total = total + stack[h * SPOTS : (h + 1) * SPOTS] * masks[h]
    return total


def head_groups(channels):
    out = []
    at = 0
    while at < channels:
        width = min(128, channels - at)
        out.append((at, width))
        at += width
    return out


def rms_stats(values):
    centre = jnp.mean(values, axis=-1, keepdims=True)
    spread = values - centre
    second = jnp.mean(spread * spread, axis=-1, keepdims=True)
    scale = lax.rsqrt(second + norm_epsilon)
    return spread * scale, scale


def norm_back(hat, scale, d_hat, count):
    first = jnp.sum(d_hat, axis=-1, keepdims=True) * (1.0 / count)
    second = jnp.sum(d_hat * hat, axis=-1, keepdims=True) * (1.0 / count)
    return scale * (d_hat - first - hat * second)


def softmax_rows(scores):
    top = jnp.max(scores, axis=-1, keepdims=True)
    weights = jnp.exp(scores - top)
    return weights / jnp.sum(weights, axis=-1, keepdims=True)


def halo_kernel(tokens, cot, lat, lon, diag, sems):
    copies = halo_copies(tokens, cot, lat, lon, diag, sems)
    for c in copies:
        c.start()
    for c in copies:
        c.wait()


def expand_bias(kinds_one, kinds_two, table_one, table_two, target, out_one, out_two, rows_ref, runs_ref):
    bands = out_one.shape[0] // LEVELS
    head_sets = [(8 * b, HEADS1) for b in range(bands)] + [(8 * bands, HEADS2)]
    width = WIN_LAT * SPAN
    slots = rows_ref.shape[0]
    rows_ref[...] = jnp.zeros(rows_ref.shape, f32)
    for b in range(bands):
        for h in range(HEADS1):
            rows_ref[8 * b + h : 8 * b + h + 1, :] = table_one[h, pl.ds(kinds_one[b], 1), :]
    for h in range(HEADS2):
        at = 8 * bands + h
        rows_ref[at : at + 1, :] = table_two[h, pl.ds(kinds_two[0], 1), :]
    runs_ref[...] = jnp.zeros(runs_ref.shape, f32)
    for z in range(LEVELS):
        for ap in range(WIN_LAT):
            start = (z * (LEVELS + 1)) * WIN_LAT * width + ap * width
            at = (z * WIN_LAT + ap) * slots
            runs_ref[at : at + slots, 0:width] = rows_ref[:, start : start + width]
    runs = runs_ref[...]
    high = runs.astype(bf16)
    rest = runs - high.astype(f32)
    middle = rest.astype(bf16)
    low = (rest - middle.astype(f32)).astype(bf16)
    sub = lax.broadcasted_iota(jnp.int32, (256, target.shape[1]), 0)
    pick = jnp.where(sub == target[0:1, :], 1.0, 0.0).astype(bf16)
    full = mm(high, pick) + mm(middle, pick) + mm(low, pick)
    lanes = lax.broadcasted_iota(jnp.int32, (1, 128), 1)
    at_end = jnp.where(lax.axis_index("lat") == lax.axis_size("lat") - 1, 1.0, 0.0).astype(f32)
    for z in range(LEVELS):
        for ap in range(WIN_LAT):
            across = jnp.where(
                (lanes >= SPOTS // 2) if ap < HALF_LAT else (lanes < SPOTS // 2), masked_score, 0.0
            )
            at = (z * WIN_LAT + ap) * slots
            for s, (first, heads) in enumerate(head_sets):
                own = across * at_end if s >= bands - 1 else jnp.zeros_like(across)
                for bp in range(WIN_LON):
                    piece = full[at + first : at + first + heads, 128 * bp : 128 * bp + 128] + own
                    spot = ap * WIN_LON + bp
                    if s < bands:
                        out_one[s * LEVELS + z, pl.ds(spot, heads, stride=SPOTS), :] = piece
                    else:
                        out_two[z, pl.ds(spot, heads, stride=SPOTS), :] = piece


def bias_call(kinds_one, kinds_two, table_one, table_two):
    bands = kinds_one.shape[0]
    target = np.full((8, WIN_LON * 128), -1, np.int32)
    for bp in range(WIN_LON):
        for aq in range(WIN_LAT):
            for bq in range(WIN_LON):
                target[:, bp * 128 + aq * WIN_LON + bq] = aq * SPAN + bp - bq + WIN_LON - 1
    slots = 8 * bands + rounded_up(HEADS2, 8)
    smem = pl.BlockSpec(memory_space=pltpu.SMEM)
    vmem = pl.BlockSpec(memory_space=pltpu.VMEM)
    return pl.pallas_call(
        expand_bias,
        name="bias",
        in_specs=[smem, smem, vmem, vmem, vmem],
        out_specs=[vmem] * 2,
        out_shape=(
            jax.ShapeDtypeStruct((bands * LEVELS, HEADS1 * SPOTS, 128), f32),
            jax.ShapeDtypeStruct((LEVELS, HEADS2 * SPOTS, 128), f32),
        ),
        scratch_shapes=[
            pltpu.VMEM((slots, table_one.shape[2]), f32),
            pltpu.VMEM((LEVELS * WIN_LAT * slots, 256), f32),
        ],
    )(kinds_one, kinds_two, table_one, table_two, target)


def halo_call(tokens, cot, lane1):
    rows, levels, lanes = tokens.shape
    low = cot.shape[0] - HALF_LAT
    return pl.pallas_call(
        halo_kernel,
        name="halo",
        in_specs=[pl.BlockSpec(memory_space=pl.ANY)] * 2,
        out_specs=[pl.BlockSpec(memory_space=pltpu.VMEM)] * 3,
        out_shape=(
            jax.ShapeDtypeStruct((HALF_LAT, levels, 2 * lanes - 3 * lane1), bf16),
            jax.ShapeDtypeStruct((rows - HALF_LAT + 2 * low, levels, lane1), bf16),
            jax.ShapeDtypeStruct((HALF_LAT, levels, 3 * lane1), bf16),
        ),
        scratch_shapes=[pltpu.SemaphoreType.DMA((7,))],
    )(tokens, cot)


def halo_copies(tokens, cot, lat, lon, diag, sems):
    rows, lanes = tokens.shape[0], tokens.shape[2]
    cut = HALF_LAT
    lane1 = diag.shape[2] // 3
    lane2 = 2 * lane1
    kept1 = lanes - lane1
    jobs = [
        (tokens.at[0:cut, :, lane1:lanes], lat.at[:, :, 0:kept1]),
        (cot.at[0:cut, :, lane2:lanes], lat.at[:, :, kept1 : kept1 + lanes - lane2]),
        (tokens.at[cut:rows, :, 0:lane1], lon.at[0 : rows - cut]),
        (tokens.at[0:cut, :, 0:lane1], diag.at[:, :, 0:lane1]),
        (cot.at[0:cut, :, 0:lane2], diag.at[:, :, lane1 : lane1 + lane2]),
    ]
    low = cot.shape[0] - cut
    for n in range(2):
        at = rows - cut + n * low
        jobs.append((cot.at[cut : cut + low, :, n * lane1 : (n + 1) * lane1], lon.at[at : at + low]))
    return [pltpu.make_async_copy(a, b, sems.at[n]) for n, (a, b) in enumerate(jobs)]


def unlace_one(main, lat, lon, diag, lace_ref, lane1):
    rows, lanes = main.shape[0], main.shape[2]
    kept = lanes - lane1
    for j in range(rows - HALF_LAT):
        lace_ref[2 * j : 2 * j + 2, 0:kept] = main[j + HALF_LAT, :, lane1:lanes].astype(f32)
        lace_ref[2 * j : 2 * j + 2, kept:lanes] = lon[j].astype(f32)
    for n in range(HALF_LAT):
        j = rows - HALF_LAT + n
        lace_ref[2 * j : 2 * j + 2, 0:kept] = lat[n, :, 0:kept].astype(f32)
        lace_ref[2 * j : 2 * j + 2, kept:lanes] = diag[n, :, 0:lane1].astype(f32)


def unlace_two(main, lat, lon, diag, lace_ref, lane1):
    rows, lanes = main.shape[0], main.shape[2]
    lane2 = 2 * lane1
    kept = lanes - lane2
    low = rows - HALF_LAT
    first = lon.shape[0] - 2 * low
    for j in range(low):
        lace_ref[2 * j : 2 * j + 2, 0:kept] = main[j + HALF_LAT, :, lane2:lanes].astype(f32)
        for n in range(2):
            at = kept + n * lane1
            lace_ref[2 * j : 2 * j + 2, at : at + lane1] = lon[first + n * low + j].astype(f32)
    for n in range(HALF_LAT):
        j = low + n
        lace_ref[2 * j : 2 * j + 2, 0:kept] = lat[n, :, lanes - lane1 : lanes - lane1 + kept].astype(f32)
        lace_ref[2 * j : 2 * j + 2, kept:lanes] = diag[n, :, lane1 : lane1 + lane2].astype(f32)


def lace_out(lace_ref, main, lat, lon, diag, cut_row, cut_lane):
    rows = main.shape[0] + cut_row
    kept = main.shape[2]
    lanes = kept + cut_lane
    for j in range(rows - cut_row):
        main[j] = lace_ref[2 * j : 2 * j + 2, 0:kept].astype(bf16)
        lon[j] = lace_ref[2 * j : 2 * j + 2, kept:lanes].astype(bf16)
    for n in range(cut_row):
        j = rows - cut_row + n
        lat[n] = lace_ref[2 * j : 2 * j + 2, 0:kept].astype(bf16)
        diag[n] = lace_ref[2 * j : 2 * j + 2, kept:lanes].astype(bf16)


def forward_one_kernel(
    main, lat, lon, diag, bias, gain, w_qkv, w_proj, index,
    out_main, out_lat, out_lon, out_diag, keep_x, keep_packed, keep_probs, keep_att,
    lace_ref, packed_ref, att_ref,
    *, cols, columns,
):
    channels = gain.shape[0]
    lace_rows = lace_ref.shape[0]
    count = lace_rows * cols
    unlace_one(main, lat, lon, diag, lace_ref, HALF_LON * channels)
    stacked = jnp.concatenate(
        [lace_ref[:, channels * k : channels * (k + 1)] for k in range(cols)], axis=0
    ).astype(bf16)
    values = mm(one_hot(index, columns[0], count, count), stacked)
    hat, _ = rms_stats(values)
    normed = (hat * gain[...][None, :]).astype(bf16)
    packed = mm(normed, w_qkv[...]).astype(bf16)
    packed_ref[...] = packed.astype(f32)
    keep_packed[...] = packed
    keep_x[...] = values.astype(bf16)
    units = count // SPOTS
    bands_span = bias.shape[0] // LEVELS
    per_band = units // bands_span
    for u in range(units):
        band, level = u // per_band, u % LEVELS
        r0 = u * SPOTS
        for at, width in head_groups(channels):
            masks = lane_head_masks(width)
            h0 = at // HEAD
            query = packed_ref[r0 : r0 + SPOTS, at : at + width]
            key = packed_ref[r0 : r0 + SPOTS, channels + at : channels + at + width].astype(bf16)
            value = packed_ref[r0 : r0 + SPOTS, 2 * channels + at : 2 * channels + at + width].astype(bf16)
            rows = slice(h0 * SPOTS, (h0 + len(masks)) * SPOTS)
            scores = mm_nt(spread_heads(query, masks).astype(bf16), key) * HEAD ** (-0.5)
            scores = scores + bias[band * LEVELS + level, rows, 0:SPOTS]
            probs = softmax_rows(scores).astype(bf16)
            keep_probs[u, rows, 0:SPOTS] = probs
            att_ref[r0 : r0 + SPOTS, at : at + width] = gather_heads(mm(probs, value), masks)
    attended = att_ref[...].astype(bf16)
    keep_att[...] = attended
    block = (values + mm(attended, w_proj[...])).astype(bf16)
    start = 0
    total = out_main.shape[0] + out_lat.shape[0] + out_lon.shape[0] + out_diag.shape[0]
    parts = mm(one_hot(index, columns[1], total, count), block).astype(bf16)
    for out in (out_main, out_lat, out_lon, out_diag):
        out[...] = parts[start : start + out.shape[0]]
        start += out.shape[0]


def merge_two_kernel(
    main, lat, lon, diag, cot_main, cot_lat, cot_lon, cot_diag, bias,
    gain_merge, gain_two, w_merge, w_qkv, w_proj, index,
    res_main, res_lat, res_lon, res_diag, d_main, d_lat, d_lon, d_diag, sums_keep, sums_send,
    lace_ref, probs_ref, packed_ref, att_ref, d_packed_ref, sums_ref,
    *, cols, columns,
):
    channels = gain_two.shape[0]
    thin = main.shape[1]
    groups = gain_merge.shape[0] // thin
    tokens = LEVELS * SPOTS
    total = main.shape[0] + lat.shape[0] + lon.shape[0] + diag.shape[0]
    stacked = jnp.concatenate([main[...], lat[...], lon[...], diag[...]], axis=0)
    grouped = mm(one_hot(index, columns[0], groups * tokens, total), stacked)
    pieces = [grouped[g * tokens : (g + 1) * tokens] for g in range(groups)]
    wide = groups * thin
    centre = sum(jnp.sum(p, axis=-1, keepdims=True) for p in pieces) * (1.0 / wide)
    spreads = [p - centre for p in pieces]
    second = sum(jnp.sum(s * s, axis=-1, keepdims=True) for s in spreads) * (1.0 / wide)
    scale_merge = lax.rsqrt(second + norm_epsilon)
    hats = [s * scale_merge for s in spreads]
    wide_gain = gain_merge[...][None, :]
    gains = [wide_gain[:, g * thin : (g + 1) * thin] for g in range(groups)]
    merged_norm = [(hats[g] * gains[g]).astype(bf16) for g in range(groups)]
    merged = mm(merged_norm[0], w_merge[0:thin, :])
    for g in range(1, groups):
        merged = merged + mm(merged_norm[g], w_merge[g * thin : (g + 1) * thin, :])
    merged = merged.astype(bf16).astype(f32)
    hat, scale_two = rms_stats(merged)
    normed = (hat * gain_two[...][None, :]).astype(bf16)
    packed_ref[...] = mm(normed, w_qkv[...]).astype(bf16).astype(f32)
    masks = lane_head_masks(128)
    per = len(masks)
    for z in range(LEVELS):
        r0 = z * SPOTS
        for at, width in head_groups(channels):
            h0 = at // HEAD
            rows = slice(h0 * SPOTS, (h0 + per) * SPOTS)
            query = packed_ref[r0 : r0 + SPOTS, at : at + width]
            key = packed_ref[r0 : r0 + SPOTS, channels + at : channels + at + width].astype(bf16)
            value = packed_ref[r0 : r0 + SPOTS, 2 * channels + at : 2 * channels + at + width].astype(bf16)
            scores = mm_nt(spread_heads(query, masks).astype(bf16), key) * HEAD ** (-0.5)
            probs = softmax_rows(scores + bias[z, rows, 0:SPOTS])
            probs_ref[z, rows, 0:SPOTS] = probs
            att_ref[r0 : r0 + SPOTS, at : at + width] = gather_heads(mm(probs.astype(bf16), value), masks)
    attended = att_ref[...].astype(bf16)
    block = (merged + mm(attended, w_proj[...])).astype(bf16)
    lace_rows = lace_ref.shape[0]
    lattice = mm(one_hot(index, columns[1], lace_rows * cols, tokens), block)
    for k in range(cols):
        lace_ref[:, channels * k : channels * (k + 1)] = lattice[lace_rows * k : lace_rows * (k + 1)]
    lace_out(lace_ref, res_main, res_lat, res_lon, res_diag, HALF_LAT, HALF_LON * channels)
    lace_ref[...] = jnp.zeros(lace_ref.shape, f32)
    unlace_two(cot_main, cot_lat, cot_lon, cot_diag, lace_ref, HALF_LON * thin)
    cot_stack = jnp.concatenate(
        [lace_ref[:, channels * k : channels * (k + 1)] for k in range(cols)], axis=0
    ).astype(bf16)
    d_block = mm(one_hot(index, columns[2], tokens, lace_rows * cols), cot_stack)
    d_block_low = d_block.astype(bf16)
    at_sum = groups * thin
    sums_ref[at_sum : at_sum + channels, :] = mm_tn(attended, d_block_low)
    att_ref[...] = mm_nt(d_block_low, w_proj[...]).astype(bf16).astype(f32)
    for z in range(LEVELS):
        r0 = z * SPOTS
        for at, width in head_groups(channels):
            h0 = at // HEAD
            rows = slice(h0 * SPOTS, (h0 + per) * SPOTS)
            attention_back(
                packed_ref, att_ref, d_packed_ref, probs_ref[z, rows, 0:SPOTS], masks, r0, at, width, channels
            )
    d_packed = d_packed_ref[...].astype(bf16)
    at_sum += channels
    for n in range(3):
        sums_ref[at_sum + n * channels : at_sum + (n + 1) * channels, :] = mm_tn(
            normed, d_packed[:, n * channels : (n + 1) * channels]
        )
    d_normed = mm_nt(d_packed, w_qkv[...]).astype(bf16).astype(f32)
    d_merged = d_block + norm_back(hat, scale_two, d_normed * gain_two[...][None, :], channels)
    d_merged = d_merged.astype(bf16)
    d_hats = []
    for g in range(groups):
        sums_ref[g * thin : (g + 1) * thin, :] = mm_tn(merged_norm[g], d_merged)
        d_norm = mm_nt(d_merged, w_merge[g * thin : (g + 1) * thin, :]).astype(bf16).astype(f32)
        d_hats.append(d_norm * gains[g])
    first = sum(jnp.sum(d, axis=-1, keepdims=True) for d in d_hats) * (1.0 / wide)
    cross = sum(jnp.sum(d * h, axis=-1, keepdims=True) for d, h in zip(d_hats, hats)) * (1.0 / wide)
    d_group = jnp.concatenate(
        [scale_merge * (d_hats[g] - first - hats[g] * cross) for g in range(groups)], axis=0
    ).astype(bf16)
    parts = mm(one_hot(index, columns[3], total, groups * tokens), d_group).astype(bf16)
    start = 0
    for out in (d_main, d_lat, d_lon, d_diag):
        out[...] = parts[start : start + out.shape[0]]
        start += out.shape[0]
    half = sums_ref.shape[0] // 2
    mine = core_of()
    first_row = pl.multiple_of(mine * half, 16)
    other_row = pl.multiple_of((1 - mine) * half, 16)
    sums_keep[...] = sums_ref[pl.ds(first_row, half), :].astype(bf16)
    sums_send[...] = sums_ref[pl.ds(other_row, half), :].astype(bf16)


def attention_back(packed_ref, d_att_ref, d_packed_ref, probs, masks, r0, at, width, channels):
    query = packed_ref[r0 : r0 + SPOTS, at : at + width]
    key = packed_ref[r0 : r0 + SPOTS, channels + at : channels + at + width].astype(bf16)
    value = packed_ref[r0 : r0 + SPOTS, 2 * channels + at : 2 * channels + at + width].astype(bf16)
    d_att = spread_heads(d_att_ref[r0 : r0 + SPOTS, at : at + width], masks).astype(bf16)
    probs_low = probs.astype(bf16)
    probs = probs.astype(f32)
    d_probs = mm_nt(d_att, value).astype(bf16).astype(f32)
    d_value = mm_tn(probs_low, d_att)
    inner = jnp.sum(probs * d_probs, axis=-1, keepdims=True)
    d_scores = (probs * (d_probs - inner) * HEAD ** (-0.5)).astype(bf16)
    d_query = gather_heads(mm(d_scores, key), masks)
    d_key = mm_tn(d_scores, spread_heads(query, masks).astype(bf16))
    d_packed_ref[r0 : r0 + SPOTS, at : at + width] = d_query
    d_packed_ref[r0 : r0 + SPOTS, channels + at : channels + at + width] = d_key
    d_packed_ref[r0 : r0 + SPOTS, 2 * channels + at : 2 * channels + at + width] = d_value


def backward_one_kernel(
    main, lat, lon, diag, keep_x, keep_packed, keep_probs, keep_att, res_lat, res_lon, res_diag,
    gain, w_qkv, w_proj, index,
    out_main, out_lat, out_lon, out_diag, sums_keep, sums_send,
    lace_ref, packed_ref, att_ref, d_packed_ref, sums_ref,
    *, cols, columns,
):
    channels = gain.shape[0]
    lace_rows = lace_ref.shape[0]
    count = lace_rows * cols
    total = main.shape[0] + lat.shape[0] + lon.shape[0] + diag.shape[0]
    stacked = jnp.concatenate([main[...], lat[...], lon[...], diag[...]], axis=0)
    d_block = mm(one_hot(index, columns[0], count, total), stacked)
    d_block_low = d_block.astype(bf16)
    hat, scale = rms_stats(keep_x[...].astype(f32))
    normed = (hat * gain[...][None, :]).astype(bf16)
    packed_ref[...] = keep_packed[...].astype(f32)
    att_ref[...] = mm_nt(d_block_low, w_proj[...]).astype(bf16).astype(f32)
    for u in range(count // SPOTS):
        r0 = u * SPOTS
        for at, width in head_groups(channels):
            masks = lane_head_masks(width)
            h0 = at // HEAD
            rows = slice(h0 * SPOTS, (h0 + len(masks)) * SPOTS)
            attention_back(
                packed_ref, att_ref, d_packed_ref, keep_probs[u, rows, 0:SPOTS], masks, r0, at, width, channels
            )
    d_packed = d_packed_ref[...].astype(bf16)
    sums_ref[:, 0 : 3 * channels] = mm_tn(normed, d_packed)
    sums_ref[:, 3 * channels : 4 * channels] = mm_tn(keep_att[...], d_block_low)
    d_normed = mm_nt(d_packed, w_qkv[...]).astype(bf16).astype(f32)
    d_shift = d_block + norm_back(hat, scale, d_normed * gain[...][None, :], channels)
    lattice = mm(one_hot(index, columns[1], count, count), d_shift.astype(bf16))
    for k in range(cols):
        lace_ref[:, channels * k : channels * (k + 1)] = lattice[lace_rows * k : lace_rows * (k + 1)]
    kept = out_main.shape[2]
    lane1 = HALF_LON * channels
    low = out_main.shape[0]
    lace_out(
        lace_ref, out_main, out_lat.at[:, :, 0:kept], out_lon.at[0:low], out_diag.at[:, :, 0:lane1],
        HALF_LAT, lane1,
    )
    out_lat[:, :, kept:] = res_lat[...]
    out_diag[:, :, lane1:] = res_diag[...]
    count = res_lon.shape[0]
    for n in range(2):
        at = low + n * count
        out_lon[at : at + count] = res_lon[:, :, n * lane1 : (n + 1) * lane1]
    mine = core_of()
    half = 2 * channels
    low = sums_ref[:, 0:half].astype(bf16)
    high = sums_ref[:, half : 2 * half].astype(bf16)

    @pl.when(mine == 0)
    def _():
        sums_keep[...] = low
        sums_send[...] = high

    @pl.when(mine != 0)
    def _():
        sums_keep[...] = high
        sums_send[...] = low


def sizes():
    return lax.axis_size("lon"), lax.axis_size("lat")


def send(values, lon_step, lat_step):
    nlon, nlat = sizes()
    route = [
        (i * nlat + j, ((i + lon_step) % nlon) * nlat + (j + lat_step) % nlat)
        for i in range(nlon)
        for j in range(nlat)
    ]
    return lax.ppermute(values, AXES, route)


def exchange(lat, lon, diag, step):
    return (send(lat, 0, step), send(lon, step, 0), send(diag, step, step))


def joined(main, lat, lon, diag):
    top = jnp.concatenate([diag, lat], axis=2)
    rest = jnp.concatenate([lon, main], axis=2)
    return jnp.concatenate([top, rest], axis=0).transpose(1, 0, 2)


def place_stages():
    nlon, nlat = sizes()
    near_lon = 2 if nlon % 4 == 0 else 1
    near_lat = 2 if nlat % 2 == 0 else 1
    far_lon = nlon // 2 // near_lon
    far_lat = nlat // near_lat

    def near(i, j, d):
        c, x, z = i % 2, i // 2 % near_lon, i // 2 // near_lon
        y, w = j % near_lat, j // near_lat
        place = (x * near_lat + y) ^ d
        return (z * near_lon + place // near_lat) * 2 + c, w * near_lat + place % near_lat

    def wide(i, j, d):
        z = i // 2 // near_lon
        return ((z + d) % far_lon) * 2 * near_lon + i % (2 * near_lon), j

    def high(i, j, d):
        return i, ((j // near_lat + d) % far_lat) * near_lat + j % near_lat

    lon_at, lat_at = lax.axis_index("lon"), lax.axis_index("lat")
    near_at = (lon_at // 2 % near_lon) * near_lat + lat_at % near_lat
    stages = [(near_lon * near_lat, near, near_at)]
    if far_lon > 1:
        stages.append((far_lon, wide, lon_at // 2 // near_lon))
    if far_lat > 1:
        stages.append((far_lat, high, lat_at // near_lat))
    return stages


def hop(values, step, d):
    nlon, nlat = sizes()
    route = []
    for i in range(nlon):
        for j in range(nlat):
            to_lon, to_lat = step(i, j, d)
            route.append((i * nlat + j, to_lon * nlat + to_lat))
    return lax.ppermute(values, AXES, route)


def pair(values):
    return hop(values, lambda i, j, d: (i ^ 1, j), 1)


def target(stage, at, d, size):
    return at ^ d if stage == 0 else (at + d) % size


def scatter(value, stages):
    for n, (size, step, at) in enumerate(stages):
        chunks = value.reshape(size, value.shape[0] // size, value.shape[1])
        total = lax.dynamic_index_in_dim(chunks, at, 0, False).astype(f32)
        got = [hop(lax.dynamic_index_in_dim(chunks, target(n, at, d, size), 0, False), step, d) for d in range(1, size)]
        for part in got:
            total = total + part.astype(f32)
        value = total.astype(bf16)
    return value


def paired(keep, sent):
    return (keep.astype(f32) + pair(sent).astype(f32)).astype(bf16)


def gather(two, one, stages):
    for n, (size, step, at) in reversed(list(enumerate(stages))):
        message = jnp.concatenate([two, one], axis=0)
        got = [message] + [hop(message, step, d) for d in range(1, size)]
        if n == 0:
            return jnp.concatenate(got, axis=0)
        rows = two.shape[0]
        two = jnp.concatenate([m[:rows] for m in got], axis=0)
        one = sum(m[rows:].astype(f32) for m in got).astype(bf16)


def finish_kernel(own, far, g_qkv_one, g_proj_one, g_merge, g_qkv_two, g_proj_two,
                  two_ref, one_ref, *, stage_sizes):
    mine = core_of()
    spots = [at for _, _, at in place_stages()]
    near = stage_sizes[0]
    span = own.shape[0] // near
    inner = two_ref.shape[0] // (2 * near)
    size = two_ref.shape[1]
    places = [jnp.int32(0)]
    width = 1
    for n in range(len(stage_sizes) - 1, 0, -1):
        count = stage_sizes[n]
        places = [lax.rem(spots[n] - d + count, count) * width + p for d in range(count) for p in places]
        width *= count
    for d in range(near):
        place = spots[0] ^ d
        for p in range(inner):
            rows = slice(d * span + p * size, d * span + (p + 1) * size)
            at = place * inner + places[p]
            two_ref[mine * near * inner + at] = own[rows, :].astype(f32)
            two_ref[(1 - mine) * near * inner + at] = far[rows, :].astype(f32)
        rows = slice(d * span + inner * size, (d + 1) * span)
        one_ref[mine * near + place] = own[rows, :].astype(f32)
        one_ref[(1 - mine) * near + place] = far[rows, :].astype(f32)

    def scale_of(parts, entries):
        total = parts[0]
        for p in parts[1:]:
            total = total + p
        return lax.rsqrt(jnp.sum(total, axis=0, keepdims=True).sum(axis=1, keepdims=True) * (1.0 / entries) + grad_epsilon)

    def spans(ref, first, last):
        rows = ref.shape[1]
        while first < last:
            n, inside = first // rows, first % rows
            size = min(rows - inside, last - first)
            yield n, inside, size, first
            first += size

    def squares(ref, first, last, lanes):
        return [
            jnp.sum(jnp.square(ref[n, i : i + s, lanes]), axis=0, keepdims=True)
            for n, i, s, _ in spans(ref, first, last)
        ]

    channels = g_proj_two.shape[0]
    wide = g_merge.shape[0]
    every = slice(0, channels)
    jobs = (
        (g_merge, [(0, wide, 0)]),
        (g_proj_two, [(wide, wide + channels, 0)]),
        (g_qkv_two, [(wide + (n + 1) * channels, wide + (n + 2) * channels, n * channels) for n in range(3)]),
    )
    for out, blocks in jobs:
        parts = [q for first, last, _ in blocks for q in squares(two_ref, first, last, every)]
        scale = scale_of(parts, out.shape[0] * out.shape[1])
        for first, last, lane in blocks:
            for n, i, s, row in spans(two_ref, first, last):
                r = row - first
                out[r : r + s, lane : lane + channels] = (two_ref[n, i : i + s, :] * scale).astype(bf16)
    thin = g_proj_one.shape[0]
    first_half = squares(one_ref, 0, thin, slice(0, 2 * thin))
    second = squares(one_ref, thin, 2 * thin, slice(0, 2 * thin))
    lanes = lax.broadcasted_iota(jnp.int32, (1, 2 * thin), 1)
    qkv_parts = first_half + [jnp.where(lanes < thin, p, 0.0) for p in second]
    proj_parts = [jnp.where(lanes < thin, 0.0, p) for p in second]
    scale_qkv = scale_of(qkv_parts, 3 * thin * thin)
    scale_proj = scale_of(proj_parts, thin * thin)
    for n, i, s, row in spans(one_ref, 0, thin):
        g_qkv_one[row : row + s, 0 : 2 * thin] = (one_ref[n, i : i + s, :] * scale_qkv).astype(bf16)
    for n, i, s, row in spans(one_ref, thin, 2 * thin):
        r = row - thin
        g_qkv_one[r : r + s, 2 * thin : 3 * thin] = (one_ref[n, i : i + s, 0:thin] * scale_qkv).astype(bf16)
        g_proj_one[r : r + s, :] = (one_ref[n, i : i + s, thin : 2 * thin] * scale_proj).astype(bf16)


def shards(
    tokens, cotangent, kinds_one, kinds_two, table_one, table_two, gain_one, gain_merge, gain_two,
    qkv_one, proj_one, merge_weight, qkv_two, proj_two,
):
    c1, c2 = proj_one.shape[0], proj_two.shape[0]
    rows1, cols1 = tokens.shape[1], tokens.shape[2] // c1
    rows2, cols2 = rows1 // 2, cols1 // 2
    nlon, nlat = sizes()
    vmem = pl.BlockSpec(memory_space=pltpu.VMEM)
    stages = place_stages()

    lace1 = lane_rows(rows1, cols1, LEVELS * rows1)
    lace2_pad = rounded_up(LEVELS * rows2, 8)
    lace2 = lane_rows(rows2, cols2, lace2_pad)
    win1, win2 = window_rows(rows1, cols1), window_rows(rows2, cols2)
    group = merge_rows(rows1, cols1)
    ahead = parts_rows(rows1, cols1, True)
    behind = parts_rows(rows1, cols1, False)
    ahead_got = moved(ahead, -HALF_LAT, -HALF_LON, rows1, cols1)
    behind_got = moved(behind, HALF_LAT, HALF_LON, rows1, cols1)
    orders = [
        index_of(win1, lace1),
        index_of(flat(ahead), win1),
        index_of(group, ahead_got),
        index_of(lace2, win2),
        index_of(win2, lace2),
        index_of(flat(behind), group),
        index_of(win1, behind_got),
        index_of(lace1, win1),
    ]
    index = np.full((max(len(o) for o in orders), 128), -1, np.int32)
    for n, order in enumerate(orders):
        index[: len(order), n] = order
    index = jnp.asarray(index)
    sizes_parts = [len(p) for p in ahead]

    lattice = tokens.transpose(1, 0, 2)
    cot = cotangent.transpose(1, 0, 2)
    halos = exchange(*halo_call(lattice, cot, HALF_LON * c1), -1)
    bias_one, bias_two = bias_call(
        kinds_one[0], kinds_two[0], table_one.swapaxes(0, 1), table_two.swapaxes(0, 1)
    )

    def part_shapes(dtype=bf16):
        return [jax.ShapeDtypeStruct((n, c1), dtype) for n in sizes_parts]

    def lace_shapes(rows, cols, channels):
        kr, kl, cl = rows - HALF_LAT, (cols - HALF_LON) * channels, HALF_LON * channels
        return [
            jax.ShapeDtypeStruct((r, LEVELS, n), bf16)
            for r, n in ((kr, kl), (HALF_LAT, kl), (kr, cl), (HALF_LAT, cl))
        ]

    count1 = LEVELS * rows1 * cols1
    units1 = count1 // SPOTS
    fwd = pl.pallas_call(
        functools.partial(forward_one_kernel, cols=cols1, columns=(0, 1)),
        name="forward_one",
        in_specs=[vmem] * 9,
        out_specs=[vmem] * 8,
        out_shape=part_shapes()
        + [
            jax.ShapeDtypeStruct((count1, c1), bf16),
            jax.ShapeDtypeStruct((count1, 3 * c1), bf16),
            jax.ShapeDtypeStruct((units1, HEADS1 * SPOTS, 128), bf16),
            jax.ShapeDtypeStruct((count1, c1), bf16),
        ],
        scratch_shapes=[
            pltpu.VMEM((LEVELS * rows1, cols1 * c1), f32),
            pltpu.VMEM((count1, 3 * c1), f32),
            pltpu.VMEM((count1, c1), f32),
        ],
    )(lattice, *halos, bias_one, gain_one, qkv_one, proj_one, index)
    parts, kept = fwd[:4], fwd[4:]
    got = exchange(*parts[1:], -1)

    tokens2 = LEVELS * SPOTS
    total_two = 4 * c1 + 4 * c2
    two = pl.pallas_call(
        functools.partial(merge_two_kernel, cols=cols2, columns=(2, 3, 4, 5)),
        name="merge_two",
        in_specs=[vmem] * 15,
        out_specs=[vmem] * 10,
        out_shape=lace_shapes(rows2, cols2, c2)
        + part_shapes()
        + [jax.ShapeDtypeStruct((total_two // 2, c2), bf16)] * 2,
        scratch_shapes=[
            pltpu.VMEM((lace2_pad, cols2 * c2), f32),
            pltpu.VMEM((LEVELS, HEADS2 * SPOTS, 128), f32),
            pltpu.VMEM((tokens2, 3 * c2), f32),
            pltpu.VMEM((tokens2, c2), f32),
            pltpu.VMEM((tokens2, 3 * c2), f32),
            pltpu.VMEM((total_two, c2), f32),
        ],
    )(parts[0], *got, cot, *halos, bias_two, gain_merge, gain_two,
      merge_weight, qkv_two, proj_two, index)
    res, d_parts, sums_two = two[:4], two[4:8], two[8:]
    half_two = paired(*sums_two)
    d_got = exchange(*d_parts[1:], 1)
    mine_two = scatter(half_two, stages)

    lanes1, lane1 = tokens.shape[2], HALF_LON * c1
    one = pl.pallas_call(
        functools.partial(backward_one_kernel, cols=cols1, columns=(6, 7)),
        name="backward_one",
        in_specs=[vmem] * 15,
        out_specs=[vmem] * 6,
        out_shape=[
            jax.ShapeDtypeStruct((rows1 - HALF_LAT, LEVELS, lanes1 - lane1), bf16),
            *(jax.ShapeDtypeStruct(h.shape, bf16) for h in halos),
        ]
        + [jax.ShapeDtypeStruct((c1, 2 * c1), bf16)] * 2,
        scratch_shapes=[
            pltpu.VMEM((LEVELS * rows1, cols1 * c1), f32),
            pltpu.VMEM((count1, 3 * c1), f32),
            pltpu.VMEM((count1, c1), f32),
            pltpu.VMEM((count1, 3 * c1), f32),
            pltpu.VMEM((c1, 4 * c1), f32),
        ],
    )(d_parts[0], *d_got, *kept, *res[1:], gain_one, qkv_one, proj_one, index)
    d_tok, sums_one = one[:4], one[4:]
    mine_one = scatter(paired(*sums_one), stages[:1])
    own = gather(mine_two, mine_one, stages)
    far = pair(own)
    lat, lon, diag = exchange(*d_tok[1:], 1)
    kept, low, cut2 = lanes1 - lane1, rows1 - HALF_LAT, rows2 - HALF_LAT
    d_tokens = joined(d_tok[0], lat[:, :, :kept], lon[:low], diag[:, :, :lane1])
    lon = jnp.concatenate([lon[low : low + cut2], lon[low + cut2 :]], axis=2)
    result = joined(res[0], lat[:, :, kept:], lon, diag[:, :, lane1:])

    near = stages[0][0]
    inner = 1
    for size, _, _ in stages[1:]:
        inner *= size
    grads = pl.pallas_call(
        functools.partial(finish_kernel, stage_sizes=tuple(size for size, _, _ in stages)),
        name="finish",
        in_specs=[vmem] * 2,
        out_specs=[vmem] * 5,
        out_shape=[
            jax.ShapeDtypeStruct(w.shape, bf16) for w in (qkv_one, proj_one, merge_weight, qkv_two, proj_two)
        ],
        scratch_shapes=[
            pltpu.VMEM((2 * near * inner,) + mine_two.shape, f32),
            pltpu.VMEM((2 * near,) + mine_one.shape, f32),
        ],
    )(own, far)
    return (result, d_tokens, *grads)


def solution(mesh):
    tiled = P(None, "lat", "lon")
    in_specs = (tiled, tiled, P(None, "lat"), P(None, "lat")) + (P(),) * 10
    out_specs = (tiled, tiled, P(), P(), P(), P(), P())

    return jax.shard_map(shards, mesh=mesh, in_specs=in_specs, out_specs=out_specs, check_vma=False)
```

```python
import functools

import jax
import jax.numpy as jnp
import numpy as np
from jax import lax
from jax.experimental import pallas as pl
from jax.experimental.pallas import tpu as pltpu
from jax.sharding import PartitionSpec as P


HEADS1 = 6
HEADS2 = 12
HEAD = 32
WIN_LAT = 6
WIN_LON = 12
HALF_LAT = WIN_LAT // 2
HALF_LON = WIN_LON // 2
SPOTS = WIN_LAT * WIN_LON
SPAN = 2 * WIN_LON - 1
LEVELS = 2

BATCH = (1, 3, 6, 8)

norm_epsilon = 1e-05
grad_epsilon = 1e-06
masked_score = -1e30

f32 = jnp.float32
bf16 = jnp.bfloat16
AXES = ("lon", "lat")


def rounded_up(count, step):
    return -(-count // step) * step


def core_of():
    return lax.axis_index("lon") % 2


def mm(a, b):
    return lax.dot_general(a, b, (((1,), (0,)), ((), ())), preferred_element_type=f32)


def mm_nt(a, b):
    return lax.dot_general(a, b, (((1,), (1,)), ((), ())), preferred_element_type=f32)


def mm_tn(a, b):
    return lax.dot_general(a, b, (((0,), (0,)), ((), ())), preferred_element_type=f32)


LIMIT = pltpu.CompilerParams(vmem_limit_bytes=24 << 20)

LIMIT_TWO = pltpu.CompilerParams(vmem_limit_bytes=24 << 20)


def near_in(*values):
    return [pltpu.with_memory_space_constraint(v, pltpu.VMEM) for v in values]


def far_in(*values):
    return [pltpu.with_memory_space_constraint(v, pltpu.HBM) for v in values]


def near_out(shapes):
    return [pltpu.VMEM(s.shape, s.dtype) for s in shapes]


def parts_rows(rows, cols, ahead):
    keep_r, keep_c = rows - HALF_LAT, cols - HALF_LON
    if ahead:
        row_sets = (range(HALF_LAT, rows), range(HALF_LAT))
        col_sets = (range(HALF_LON, cols), range(HALF_LON))
    else:
        row_sets = (range(keep_r), range(keep_r, rows))
        col_sets = (range(keep_c), range(keep_c, cols))
    out = []
    for rset, cset in ((0, 0), (1, 0), (0, 1), (1, 1)):
        piece = [(z, j, k) for z in range(LEVELS) for j in row_sets[rset] for k in col_sets[cset]]
        piece += [None] * (rounded_up(len(piece), 16) - len(piece))
        out.append(piece)
    return out


def window_rows(rows, cols):
    return [
        (z, b * WIN_LAT + ap, c * WIN_LON + bp)
        for b in range(rows // WIN_LAT)
        for c in range(cols // WIN_LON)
        for z in range(LEVELS)
        for ap in range(WIN_LAT)
        for bp in range(WIN_LON)
    ]


def merge_rows(rows, cols):
    return [
        (z, 2 * jj + a, 2 * kk + b)
        for a in range(2)
        for b in range(2)
        for z in range(LEVELS)
        for jj in range(rows // 2)
        for kk in range(cols // 2)
    ]


def lane_rows(rows, cols, pad):
    out = []
    for k in range(cols):
        group = [(1 - z, j, k) for j in range(rows) for z in range(LEVELS)]
        out += group + [None] * (pad - len(group))
    return out


def index_of(wanted, source):
    where = {spot: n for n, spot in enumerate(source) if spot is not None}
    return [-1 if spot is None else where[spot] for spot in wanted]


def flat(pieces):
    return [spot for piece in pieces for spot in piece]


def moved(pieces, dj, dk, rows, cols):
    return [
        None if s is None else (s[0], (s[1] + dj) % rows, (s[2] + dk) % cols) for s in flat(pieces)
    ]


def one_hot(index_ref, column, count, width):
    index = index_ref[0:count, column : column + 1]
    lanes = lax.broadcasted_iota(jnp.int32, (count, width), 1)
    return jnp.where(index == lanes, 1.0, 0.0).astype(bf16)


def lane_head_masks(width):
    lanes = lax.broadcasted_iota(jnp.int32, (1, width), 1)
    return [
        jnp.where((lanes >= h * HEAD) & (lanes < (h + 1) * HEAD), 1.0, 0.0).astype(f32)
        for h in range(width // HEAD)
    ]


def spread_heads(values, masks):
    return jnp.concatenate([values * m for m in masks], axis=0)


def gather_heads(stack, masks):
    total = stack[0:SPOTS] * masks[0]
    for h in range(1, len(masks)):
        total = total + stack[h * SPOTS : (h + 1) * SPOTS] * masks[h]
    return total


def head_groups(channels):
    out = []
    at = 0
    while at < channels:
        width = min(128, channels - at)
        out.append((at, width))
        at += width
    return out


def rms_stats(values):
    centre = jnp.mean(values, axis=-1, keepdims=True)
    spread = values - centre
    second = jnp.mean(spread * spread, axis=-1, keepdims=True)
    scale = lax.rsqrt(second + norm_epsilon)
    return spread * scale, scale


def norm_back(hat, scale, d_hat, count):
    first = jnp.sum(d_hat, axis=-1, keepdims=True) * (1.0 / count)
    second = jnp.sum(d_hat * hat, axis=-1, keepdims=True) * (1.0 / count)
    return scale * (d_hat - first - hat * second)


def softmax_rows(scores):
    top = jnp.max(scores, axis=-1, keepdims=True)
    weights = jnp.exp(scores - top)
    return weights / jnp.sum(weights, axis=-1, keepdims=True)


def halo_kernel(tokens, cot, lat, lon, diag, sems):
    copies = halo_copies(tokens, cot, lat, lon, diag, sems)
    for c in copies:
        c.start()
    for c in copies:
        c.wait()


def expand_bias(kinds_one, kinds_two, table_one, table_two, target, out_one, out_two, rows_ref, runs_ref):
    bands = out_one.shape[0] // LEVELS
    head_sets = [(8 * b, HEADS1) for b in range(bands)] + [(8 * bands, HEADS2)]
    width = WIN_LAT * SPAN
    slots = rows_ref.shape[0]
    rows_ref[...] = jnp.zeros(rows_ref.shape, f32)
    for b in range(bands):
        for h in range(HEADS1):
            rows_ref[8 * b + h : 8 * b + h + 1, :] = table_one[h, pl.ds(kinds_one[0, b], 1), :]
    for h in range(HEADS2):
        at = 8 * bands + h
        rows_ref[at : at + 1, :] = table_two[h, pl.ds(kinds_two[0, 0], 1), :]
    runs_ref[...] = jnp.zeros(runs_ref.shape, f32)
    for z in range(LEVELS):
        for ap in range(WIN_LAT):
            start = (z * (LEVELS + 1)) * WIN_LAT * width + ap * width
            at = (z * WIN_LAT + ap) * slots
            runs_ref[at : at + slots, 0:width] = rows_ref[:, start : start + width]
    runs = runs_ref[...]
    high = runs.astype(bf16)
    rest = runs - high.astype(f32)
    middle = rest.astype(bf16)
    low = (rest - middle.astype(f32)).astype(bf16)
    sub = lax.broadcasted_iota(jnp.int32, (256, target.shape[1]), 0)
    pick = jnp.where(sub == target[0:1, :], 1.0, 0.0).astype(bf16)
    full = mm(high, pick) + mm(middle, pick) + mm(low, pick)
    lanes = lax.broadcasted_iota(jnp.int32, (1, 128), 1)
    at_end = jnp.where(lax.axis_index("lat") == lax.axis_size("lat") - 1, 1.0, 0.0).astype(f32)
    for z in range(LEVELS):
        for ap in range(WIN_LAT):
            across = jnp.where(
                (lanes >= SPOTS // 2) if ap < HALF_LAT else (lanes < SPOTS // 2), masked_score, 0.0
            )
            at = (z * WIN_LAT + ap) * slots
            for s, (first, heads) in enumerate(head_sets):
                own = across * at_end if s >= bands - 1 else jnp.zeros_like(across)
                for bp in range(WIN_LON):
                    piece = full[at + first : at + first + heads, 128 * bp : 128 * bp + 128] + own
                    spot = ap * WIN_LON + bp
                    if s < bands:
                        out_one[s * LEVELS + z, pl.ds(spot, heads, stride=SPOTS), :] = piece
                    else:
                        out_two[z, pl.ds(spot, heads, stride=SPOTS), :] = piece


def bias_call(kinds_one, kinds_two, table_one, table_two):
    bands = kinds_one.shape[1]
    target = np.full((8, WIN_LON * 128), -1, np.int32)
    for bp in range(WIN_LON):
        for aq in range(WIN_LAT):
            for bq in range(WIN_LON):
                target[:, bp * 128 + aq * WIN_LON + bq] = aq * SPAN + bp - bq + WIN_LON - 1
    slots = 8 * bands + rounded_up(HEADS2, 8)
    smem = pl.BlockSpec(memory_space=pltpu.SMEM)
    vmem = pl.BlockSpec(memory_space=pltpu.VMEM)
    return pl.pallas_call(
        expand_bias,
        name="bias",
        in_specs=[smem, smem, vmem, vmem, vmem],
        out_specs=[vmem] * 2,
        out_shape=(
            pltpu.VMEM((bands * LEVELS, HEADS1 * SPOTS, 128), f32),
            pltpu.VMEM((LEVELS, HEADS2 * SPOTS, 128), f32),
        ),
        compiler_params=LIMIT,
        scratch_shapes=[
            pltpu.VMEM((slots, table_one.shape[2]), f32),
            pltpu.VMEM((LEVELS * WIN_LAT * slots, 256), f32),
        ],
    )(kinds_one, kinds_two, *far_in(table_one, table_two, jnp.asarray(target)))


def halo_call(tokens, cot, lane1):
    rows, levels, lanes = tokens.shape
    low = cot.shape[0] - HALF_LAT
    return pl.pallas_call(
        halo_kernel,
        name="halo",
        in_specs=[pl.BlockSpec(memory_space=pl.ANY)] * 2,
        out_specs=[pl.BlockSpec(memory_space=pltpu.VMEM)] * 3,
        out_shape=(
            pltpu.VMEM((HALF_LAT, levels, 2 * lanes - 3 * lane1), bf16),
            pltpu.VMEM((rows - HALF_LAT + 2 * low, levels, lane1), bf16),
            pltpu.VMEM((HALF_LAT, levels, 3 * lane1), bf16),
        ),
        compiler_params=LIMIT,
        scratch_shapes=[pltpu.SemaphoreType.DMA((7,))],
    )(*far_in(tokens, cot))


def halo_copies(tokens, cot, lat, lon, diag, sems):
    rows, lanes = tokens.shape[0], tokens.shape[2]
    cut = HALF_LAT
    lane1 = diag.shape[2] // 3
    lane2 = 2 * lane1
    kept1 = lanes - lane1
    jobs = [
        (tokens.at[0:cut, :, lane1:lanes], lat.at[:, :, 0:kept1]),
        (cot.at[0:cut, :, lane2:lanes], lat.at[:, :, kept1 : kept1 + lanes - lane2]),
        (tokens.at[cut:rows, :, 0:lane1], lon.at[0 : rows - cut]),
        (tokens.at[0:cut, :, 0:lane1], diag.at[:, :, 0:lane1]),
        (cot.at[0:cut, :, 0:lane2], diag.at[:, :, lane1 : lane1 + lane2]),
    ]
    low = cot.shape[0] - cut
    for n in range(2):
        at = rows - cut + n * low
        jobs.append((cot.at[cut : cut + low, :, n * lane1 : (n + 1) * lane1], lon.at[at : at + low]))
    return [pltpu.make_async_copy(a, b, sems.at[n]) for n, (a, b) in enumerate(jobs)]


def unlace_one(main, lat, lon, diag, lace_ref, lane1):
    rows, lanes = main.shape[0], main.shape[2]
    kept = lanes - lane1
    for j in range(rows - HALF_LAT):
        lace_ref[2 * j : 2 * j + 2, 0:kept] = main[j + HALF_LAT, :, lane1:lanes].astype(f32)
        lace_ref[2 * j : 2 * j + 2, kept:lanes] = lon[j].astype(f32)
    for n in range(HALF_LAT):
        j = rows - HALF_LAT + n
        lace_ref[2 * j : 2 * j + 2, 0:kept] = lat[n, :, 0:kept].astype(f32)
        lace_ref[2 * j : 2 * j + 2, kept:lanes] = diag[n, :, 0:lane1].astype(f32)


def unlace_two(main, lat, lon, diag, lace_ref, lane1):
    rows, lanes = main.shape[0], main.shape[2]
    lane2 = 2 * lane1
    kept = lanes - lane2
    low = rows - HALF_LAT
    first = lon.shape[0] - 2 * low
    for j in range(low):
        lace_ref[2 * j : 2 * j + 2, 0:kept] = main[j + HALF_LAT, :, lane2:lanes].astype(f32)
        for n in range(2):
            at = kept + n * lane1
            lace_ref[2 * j : 2 * j + 2, at : at + lane1] = lon[first + n * low + j].astype(f32)
    for n in range(HALF_LAT):
        j = low + n
        lace_ref[2 * j : 2 * j + 2, 0:kept] = lat[n, :, lanes - lane1 : lanes - lane1 + kept].astype(f32)
        lace_ref[2 * j : 2 * j + 2, kept:lanes] = diag[n, :, lane1 : lane1 + lane2].astype(f32)


def lace_out(lace_ref, main, lat, lon, diag, cut_row, cut_lane):
    rows = main.shape[0] + cut_row
    kept = main.shape[2]
    lanes = kept + cut_lane
    for j in range(rows - cut_row):
        main[j] = lace_ref[2 * j : 2 * j + 2, 0:kept].astype(bf16)
        lon[j] = lace_ref[2 * j : 2 * j + 2, kept:lanes].astype(bf16)
    for n in range(cut_row):
        j = rows - cut_row + n
        lat[n] = lace_ref[2 * j : 2 * j + 2, 0:kept].astype(bf16)
        diag[n] = lace_ref[2 * j : 2 * j + 2, kept:lanes].astype(bf16)


def forward_one_kernel(
    main, lat, lon, diag, bias, gain, w_qkv, w_proj, index,
    out_main, out_lat, out_lon, out_diag, keep_x, keep_packed, keep_probs, keep_att,
    lace_ref, packed_ref, att_ref,
    *, cols, columns,
):
    channels = gain.shape[0]
    lace_rows = lace_ref.shape[0]
    count = lace_rows * cols
    unlace_one(main, lat, lon, diag, lace_ref, HALF_LON * channels)
    stacked = jnp.concatenate(
        [lace_ref[:, channels * k : channels * (k + 1)] for k in range(cols)], axis=0
    ).astype(bf16)
    values = mm(one_hot(index, columns[0], count, count), stacked)
    hat, _ = rms_stats(values)
    normed = (hat * gain[...][None, :]).astype(bf16)
    packed = mm(normed, w_qkv[...]).astype(bf16)
    packed_ref[...] = packed.astype(f32)
    keep_packed[...] = packed
    keep_x[...] = values.astype(bf16)
    units = count // SPOTS
    bands_span = bias.shape[0] // LEVELS
    per_band = units // bands_span

    def bias_of(key_of):
        u, rows = key_of
        return bias[u // per_band * LEVELS + u % LEVELS, rows, 0:SPOTS]

    def keep(key_of, weights):
        u, rows = key_of
        keep_probs[u, rows, 0:SPOTS] = weights.astype(bf16)

    attention(packed_ref, att_ref, bias_of, keep, head_jobs(units, channels), channels, BATCH[0])
    attended = att_ref[...].astype(bf16)
    keep_att[...] = attended
    block = (values + mm(attended, w_proj[...])).astype(bf16)
    start = 0
    total = out_main.shape[0] + out_lat.shape[0] + out_lon.shape[0] + out_diag.shape[0]
    parts = mm(one_hot(index, columns[1], total, count), block).astype(bf16)
    for out in (out_main, out_lat, out_lon, out_diag):
        out[...] = parts[start : start + out.shape[0]]
        start += out.shape[0]


def merge_two_kernel(
    main, lat, lon, diag, cot_main, cot_lat, cot_lon, cot_diag, bias,
    gain_merge, gain_two, w_merge, w_qkv, w_proj, index,
    res_main, res_lat, res_lon, res_diag, d_main, d_lat, d_lon, d_diag, sums_keep, sums_send,
    lace_ref, probs_ref, packed_ref, att_ref, d_packed_ref, sums_ref,
    *, cols, columns,
):
    channels = gain_two.shape[0]
    thin = main.shape[1]
    groups = gain_merge.shape[0] // thin
    tokens = LEVELS * SPOTS
    total = main.shape[0] + lat.shape[0] + lon.shape[0] + diag.shape[0]
    stacked = jnp.concatenate([main[...], lat[...], lon[...], diag[...]], axis=0)
    grouped = mm(one_hot(index, columns[0], groups * tokens, total), stacked)
    pieces = [grouped[g * tokens : (g + 1) * tokens] for g in range(groups)]
    wide = groups * thin
    centre = sum(jnp.sum(p, axis=-1, keepdims=True) for p in pieces) * (1.0 / wide)
    spreads = [p - centre for p in pieces]
    second = sum(jnp.sum(s * s, axis=-1, keepdims=True) for s in spreads) * (1.0 / wide)
    scale_merge = lax.rsqrt(second + norm_epsilon)
    hats = [s * scale_merge for s in spreads]
    wide_gain = gain_merge[...][None, :]
    gains = [wide_gain[:, g * thin : (g + 1) * thin] for g in range(groups)]
    merged_norm = [(hats[g] * gains[g]).astype(bf16) for g in range(groups)]
    merged = mm(merged_norm[0], w_merge[0:thin, :])
    for g in range(1, groups):
        merged = merged + mm(merged_norm[g], w_merge[g * thin : (g + 1) * thin, :])
    merged = merged.astype(bf16).astype(f32)
    hat, scale_two = rms_stats(merged)
    normed = (hat * gain_two[...][None, :]).astype(bf16)
    packed_ref[...] = mm(normed, w_qkv[...]).astype(bf16).astype(f32)

    def keep(key_of, weights):
        probs_ref[key_of[0], key_of[1], 0:SPOTS] = weights

    jobs = head_jobs(LEVELS, channels)
    attention(
        packed_ref, att_ref, lambda k: bias[k[0], k[1], 0:SPOTS], keep, jobs, channels, BATCH[1]
    )
    attended = att_ref[...].astype(bf16)
    block = (merged + mm(attended, w_proj[...])).astype(bf16)
    lace_rows = lace_ref.shape[0]
    lattice = mm(one_hot(index, columns[1], lace_rows * cols, tokens), block)
    for k in range(cols):
        lace_ref[:, channels * k : channels * (k + 1)] = lattice[lace_rows * k : lace_rows * (k + 1)]
    lace_out(lace_ref, res_main, res_lat, res_lon, res_diag, HALF_LAT, HALF_LON * channels)
    lace_ref[...] = jnp.zeros(lace_ref.shape, f32)
    unlace_two(cot_main, cot_lat, cot_lon, cot_diag, lace_ref, HALF_LON * thin)
    cot_stack = jnp.concatenate(
        [lace_ref[:, channels * k : channels * (k + 1)] for k in range(cols)], axis=0
    ).astype(bf16)
    d_block = mm(one_hot(index, columns[2], tokens, lace_rows * cols), cot_stack)
    d_block_low = d_block.astype(bf16)
    at_sum = groups * thin
    sums_ref[at_sum : at_sum + channels, :] = mm_tn(attended, d_block_low)
    att_ref[...] = mm_nt(d_block_low, w_proj[...]).astype(bf16).astype(f32)
    attention_back(
        packed_ref, att_ref, d_packed_ref, lambda k: probs_ref[k[0], k[1], 0:SPOTS], jobs, channels, BATCH[2]
    )
    d_packed = d_packed_ref[...].astype(bf16)
    at_sum += channels
    for n in range(3):
        sums_ref[at_sum + n * channels : at_sum + (n + 1) * channels, :] = mm_tn(
            normed, d_packed[:, n * channels : (n + 1) * channels]
        )
    d_normed = mm_nt(d_packed, w_qkv[...]).astype(bf16).astype(f32)
    d_merged = d_block + norm_back(hat, scale_two, d_normed * gain_two[...][None, :], channels)
    d_merged = d_merged.astype(bf16)
    d_hats = []
    for g in range(groups):
        sums_ref[g * thin : (g + 1) * thin, :] = mm_tn(merged_norm[g], d_merged)
        d_norm = mm_nt(d_merged, w_merge[g * thin : (g + 1) * thin, :]).astype(bf16).astype(f32)
        d_hats.append(d_norm * gains[g])
    first = sum(jnp.sum(d, axis=-1, keepdims=True) for d in d_hats) * (1.0 / wide)
    cross = sum(jnp.sum(d * h, axis=-1, keepdims=True) for d, h in zip(d_hats, hats)) * (1.0 / wide)
    d_group = jnp.concatenate(
        [scale_merge * (d_hats[g] - first - hats[g] * cross) for g in range(groups)], axis=0
    ).astype(bf16)
    parts = mm(one_hot(index, columns[3], total, groups * tokens), d_group).astype(bf16)
    start = 0
    for out in (d_main, d_lat, d_lon, d_diag):
        out[...] = parts[start : start + out.shape[0]]
        start += out.shape[0]
    half = sums_ref.shape[0] // 2
    mine = core_of()
    first_row = pl.multiple_of(mine * half, 16)
    other_row = pl.multiple_of((1 - mine) * half, 16)
    sums_keep[...] = sums_ref[pl.ds(first_row, half), :].astype(bf16)
    sums_send[...] = sums_ref[pl.ds(other_row, half), :].astype(bf16)


def qkv_of(packed_ref, r0, at, width, channels):
    rows = slice(r0, r0 + SPOTS)
    query = packed_ref[rows, at : at + width]
    key = packed_ref[rows, channels + at : channels + at + width].astype(bf16)
    value = packed_ref[rows, 2 * channels + at : 2 * channels + at + width].astype(bf16)
    return query, key, value


def batches(jobs, size):
    return [jobs[n : n + size] for n in range(0, len(jobs), size)]


def attention_back(packed_ref, d_att_ref, d_packed_ref, probs_of, jobs, channels, size):
    for batch in batches(jobs, size):
        state = []
        for r0, at, width, key_of in batch:
            masks = lane_head_masks(width)
            value = qkv_of(packed_ref, r0, at, width, channels)[2]
            d_att = spread_heads(d_att_ref[r0 : r0 + SPOTS, at : at + width], masks).astype(bf16)
            state.append((d_att, mm_nt(d_att, value)))
        scores = []
        for (r0, at, width, key_of), (d_att, d_probs) in zip(batch, state):
            probs = probs_of(key_of).astype(f32)
            d_probs = d_probs.astype(bf16).astype(f32)
            inner = jnp.sum(probs * d_probs, axis=-1, keepdims=True)
            scores.append((probs * (d_probs - inner) * HEAD ** (-0.5)).astype(bf16))
        for (r0, at, width, key_of), (d_att, _), d_scores in zip(batch, state, scores):
            masks = lane_head_masks(width)
            query, key, _ = qkv_of(packed_ref, r0, at, width, channels)
            rows = slice(r0, r0 + SPOTS)
            d_packed_ref[rows, at : at + width] = gather_heads(mm(d_scores, key), masks)
            d_packed_ref[rows, channels + at : channels + at + width] = mm_tn(
                d_scores, spread_heads(query, masks).astype(bf16)
            )
            d_packed_ref[rows, 2 * channels + at : 2 * channels + at + width] = mm_tn(
                probs_of(key_of).astype(bf16), d_att
            )


def attention(packed_ref, att_ref, bias_of, keep, jobs, channels, size):
    for batch in batches(jobs, size):
        scores = []
        for r0, at, width, key_of in batch:
            masks = lane_head_masks(width)
            query, key, _ = qkv_of(packed_ref, r0, at, width, channels)
            scores.append(mm_nt(spread_heads(query, masks).astype(bf16), key))
        probs = []
        for (r0, at, width, key_of), score in zip(batch, scores):
            weights = softmax_rows(score * HEAD ** (-0.5) + bias_of(key_of))
            keep(key_of, weights)
            probs.append(weights.astype(bf16))
        for (r0, at, width, key_of), weights in zip(batch, probs):
            value = qkv_of(packed_ref, r0, at, width, channels)[2]
            att_ref[r0 : r0 + SPOTS, at : at + width] = gather_heads(
                mm(weights, value), lane_head_masks(width)
            )


def head_jobs(units, channels):
    return [
        (u * SPOTS, at, width, (u, slice(at // HEAD * SPOTS, (at + width) // HEAD * SPOTS)))
        for u in range(units)
        for at, width in head_groups(channels)
    ]


def backward_one_kernel(
    main, lat, lon, diag, keep_x, keep_packed, keep_probs, keep_att, res_lat, res_lon, res_diag,
    gain, w_qkv, w_proj, index,
    out_main, out_lat, out_lon, out_diag, sums_keep, sums_send,
    lace_ref, packed_ref, att_ref, d_packed_ref, sums_ref,
    *, cols, columns,
):
    channels = gain.shape[0]
    lace_rows = lace_ref.shape[0]
    count = lace_rows * cols
    total = main.shape[0] + lat.shape[0] + lon.shape[0] + diag.shape[0]
    stacked = jnp.concatenate([main[...], lat[...], lon[...], diag[...]], axis=0)
    d_block = mm(one_hot(index, columns[0], count, total), stacked)
    d_block_low = d_block.astype(bf16)
    hat, scale = rms_stats(keep_x[...].astype(f32))
    normed = (hat * gain[...][None, :]).astype(bf16)
    packed_ref[...] = keep_packed[...].astype(f32)
    att_ref[...] = mm_nt(d_block_low, w_proj[...]).astype(bf16).astype(f32)
    attention_back(
        packed_ref, att_ref, d_packed_ref, lambda k: keep_probs[k[0], k[1], 0:SPOTS],
        head_jobs(count // SPOTS, channels), channels, BATCH[3],
    )
    d_packed = d_packed_ref[...].astype(bf16)
    sums_ref[:, 0 : 3 * channels] = mm_tn(normed, d_packed)
    sums_ref[:, 3 * channels : 4 * channels] = mm_tn(keep_att[...], d_block_low)
    d_normed = mm_nt(d_packed, w_qkv[...]).astype(bf16).astype(f32)
    d_shift = d_block + norm_back(hat, scale, d_normed * gain[...][None, :], channels)
    lattice = mm(one_hot(index, columns[1], count, count), d_shift.astype(bf16))
    for k in range(cols):
        lace_ref[:, channels * k : channels * (k + 1)] = lattice[lace_rows * k : lace_rows * (k + 1)]
    kept = out_main.shape[2]
    lane1 = HALF_LON * channels
    low = out_main.shape[0]
    lace_out(
        lace_ref, out_main, out_lat.at[:, :, 0:kept], out_lon.at[0:low], out_diag.at[:, :, 0:lane1],
        HALF_LAT, lane1,
    )
    out_lat[:, :, kept:] = res_lat[...]
    out_diag[:, :, lane1:] = res_diag[...]
    count = res_lon.shape[0]
    for n in range(2):
        at = low + n * count
        out_lon[at : at + count] = res_lon[:, :, n * lane1 : (n + 1) * lane1]
    mine = core_of()
    half = 2 * channels
    low = sums_ref[:, 0:half].astype(bf16)
    high = sums_ref[:, half : 2 * half].astype(bf16)

    @pl.when(mine == 0)
    def _():
        sums_keep[...] = low
        sums_send[...] = high

    @pl.when(mine != 0)
    def _():
        sums_keep[...] = high
        sums_send[...] = low


def sizes():
    return lax.axis_size("lon"), lax.axis_size("lat")


def send(values, lon_step, lat_step):
    nlon, nlat = sizes()
    route = [
        (i * nlat + j, ((i + lon_step) % nlon) * nlat + (j + lat_step) % nlat)
        for i in range(nlon)
        for j in range(nlat)
    ]
    return lax.ppermute(values, AXES, route)


def exchange(lat, lon, diag, step):
    return (send(lat, 0, step), send(lon, step, 0), send(diag, step, step))


def join_kernel(res_main, d_main, lat, lon, diag, result, d_tokens):
    rows, lanes = d_tokens.shape[0], d_tokens.shape[2]
    cut = HALF_LAT
    kept = d_main.shape[2]
    lane1 = lanes - kept
    d_tokens[cut:rows, :, lane1:lanes] = d_main[...]
    d_tokens[0:cut, :, lane1:lanes] = lat[:, :, 0:kept]
    d_tokens[cut:rows, :, 0:lane1] = lon[0 : rows - cut]
    d_tokens[0:cut, :, 0:lane1] = diag[:, :, 0:lane1]
    low = res_main.shape[0]
    lane2 = 2 * lane1
    result[cut : cut + low, :, lane2:lanes] = res_main[...]
    result[0:cut, :, lane2:lanes] = lat[:, :, kept:]
    result[0:cut, :, 0:lane2] = diag[:, :, lane1:]
    for n in range(2):
        at = rows - cut + n * low
        result[cut : cut + low, :, n * lane1 : (n + 1) * lane1] = lon[at : at + low]


def place_stages():
    nlon, nlat = sizes()
    near_lon = 2 if nlon % 4 == 0 else 1
    near_lat = 2 if nlat % 2 == 0 else 1
    far_lon = nlon // 2 // near_lon
    far_lat = nlat // near_lat

    def near(i, j, d):
        c, x, z = i % 2, i // 2 % near_lon, i // 2 // near_lon
        y, w = j % near_lat, j // near_lat
        place = (x * near_lat + y) ^ d
        return (z * near_lon + place // near_lat) * 2 + c, w * near_lat + place % near_lat

    def wide(i, j, d):
        z = i // 2 // near_lon
        return ((z + d) % far_lon) * 2 * near_lon + i % (2 * near_lon), j

    def high(i, j, d):
        return i, ((j // near_lat + d) % far_lat) * near_lat + j % near_lat

    lon_at, lat_at = lax.axis_index("lon"), lax.axis_index("lat")
    near_at = (lon_at // 2 % near_lon) * near_lat + lat_at % near_lat
    stages = [(near_lon * near_lat, near, near_at)]
    if far_lon > 1:
        stages.append((far_lon, wide, lon_at // 2 // near_lon))
    if far_lat > 1:
        stages.append((far_lat, high, lat_at // near_lat))
    return stages


def hop(values, step, d):
    nlon, nlat = sizes()
    route = []
    for i in range(nlon):
        for j in range(nlat):
            to_lon, to_lat = step(i, j, d)
            route.append((i * nlat + j, to_lon * nlat + to_lat))
    return lax.ppermute(values, AXES, route)


def pair(values):
    return hop(values, lambda i, j, d: (i ^ 1, j), 1)


def target(stage, at, d, size):
    return at ^ d if stage == 0 else (at + d) % size


def total_of(refs, rows):
    total = refs[0][rows, :].astype(f32)
    for r in refs[1:]:
        total = total + r[rows, :].astype(f32)
    return total


def split_kernel(*refs, count, stage):
    size, _, at = place_stages()[stage]
    outs, scratch = refs[count:-1], refs[-1]
    rows = scratch.shape[1]
    for p in range(size):
        scratch[p] = total_of(refs[:count], slice(p * rows, (p + 1) * rows))
    for d in range(size):
        outs[d][...] = scratch[target(stage, at, d, size)].astype(bf16)


def sum_split(values, stage):
    size = place_stages()[stage][0]
    rows, width = values[0].shape
    vmem = pl.BlockSpec(memory_space=pltpu.VMEM)
    return pl.pallas_call(
        functools.partial(split_kernel, count=len(values), stage=stage),
        in_specs=[vmem] * len(values),
        out_specs=[vmem] * size,
        out_shape=[pltpu.VMEM((rows // size, width), bf16)] * size,
        scratch_shapes=[pltpu.VMEM((size, rows // size, width), f32)],
        compiler_params=LIMIT,
    )(*near_in(*values))


def message_kernel(*refs, count):
    out = refs[-1]
    rows = refs[0].shape[0]
    out[0:rows, :] = total_of(refs[:count], slice(0, rows)).astype(bf16)
    small = refs[count].shape[0]
    out[rows : rows + small, :] = total_of(refs[count:-1], slice(0, small)).astype(bf16)


def message_of(two, one):
    vmem = pl.BlockSpec(memory_space=pltpu.VMEM)
    values = [*two, *one]
    return pl.pallas_call(
        functools.partial(message_kernel, count=len(two)),
        name="message",
        in_specs=[vmem] * len(values),
        out_specs=vmem,
        out_shape=pltpu.VMEM((two[0].shape[0] + one[0].shape[0], two[0].shape[1]), bf16),
        compiler_params=LIMIT,
    )(*near_in(*values))


def widen_kernel(*refs, rows):
    out, ins = refs[-1], refs[:-1]
    for n, r in enumerate(ins):
        out[n * rows : (n + 1) * rows, :] = r[0:rows, :]
    total = ins[0].shape[0]
    out[len(ins) * rows :, :] = total_of(ins, slice(rows, total)).astype(bf16)


def widen(messages, small):
    vmem = pl.BlockSpec(memory_space=pltpu.VMEM)
    rows = messages[0].shape[0] - small
    return pl.pallas_call(
        functools.partial(widen_kernel, rows=rows),
        name="widen",
        in_specs=[vmem] * len(messages),
        out_specs=vmem,
        out_shape=pltpu.VMEM((rows * len(messages) + small, messages[0].shape[1]), bf16),
        compiler_params=LIMIT,
    )(*near_in(*messages))


def moves(values, stage):
    size, step, _ = place_stages()[stage]
    return [values[0]] + [hop(values[d], step, d) for d in range(1, size)]


def finish_kernel(*refs, stage_sizes):
    near = stage_sizes[0]
    own, far = refs[:near], refs[near : 2 * near]
    g_qkv_one, g_proj_one, g_merge, g_qkv_two, g_proj_two, two_ref, one_ref = refs[2 * near :]
    mine = core_of()
    spots = [at for _, _, at in place_stages()]
    inner = two_ref.shape[0] // (2 * near)
    size = two_ref.shape[1]
    places = [jnp.int32(0)]
    width = 1
    for n in range(len(stage_sizes) - 1, 0, -1):
        count = stage_sizes[n]
        places = [lax.rem(spots[n] - d + count, count) * width + p for d in range(count) for p in places]
        width *= count
    for d in range(near):
        place = spots[0] ^ d
        for p in range(inner):
            rows = slice(p * size, (p + 1) * size)
            at = place * inner + places[p]
            two_ref[mine * near * inner + at] = own[d][rows, :].astype(f32)
            two_ref[(1 - mine) * near * inner + at] = far[d][rows, :].astype(f32)
        rows = slice(inner * size, own[d].shape[0])
        one_ref[mine * near + place] = own[d][rows, :].astype(f32)
        one_ref[(1 - mine) * near + place] = far[d][rows, :].astype(f32)

    def scale_of(parts, entries):
        total = parts[0]
        for p in parts[1:]:
            total = total + p
        return lax.rsqrt(jnp.sum(total, axis=0, keepdims=True).sum(axis=1, keepdims=True) * (1.0 / entries) + grad_epsilon)

    def spans(ref, first, last):
        rows = ref.shape[1]
        while first < last:
            n, inside = first // rows, first % rows
            size = min(rows - inside, last - first)
            yield n, inside, size, first
            first += size

    def squares(ref, first, last, lanes):
        return [
            jnp.sum(jnp.square(ref[n, i : i + s, lanes]), axis=0, keepdims=True)
            for n, i, s, _ in spans(ref, first, last)
        ]

    channels = g_proj_two.shape[0]
    wide = g_merge.shape[0]
    every = slice(0, channels)
    jobs = (
        (g_merge, [(0, wide, 0)]),
        (g_proj_two, [(wide, wide + channels, 0)]),
        (g_qkv_two, [(wide + (n + 1) * channels, wide + (n + 2) * channels, n * channels) for n in range(3)]),
    )
    for out, blocks in jobs:
        parts = [q for first, last, _ in blocks for q in squares(two_ref, first, last, every)]
        scale = scale_of(parts, out.shape[0] * out.shape[1])
        for first, last, lane in blocks:
            for n, i, s, row in spans(two_ref, first, last):
                r = row - first
                out[r : r + s, lane : lane + channels] = (two_ref[n, i : i + s, :] * scale).astype(bf16)
    thin = g_proj_one.shape[0]
    first_half = squares(one_ref, 0, thin, slice(0, 2 * thin))
    second = squares(one_ref, thin, 2 * thin, slice(0, 2 * thin))
    lanes = lax.broadcasted_iota(jnp.int32, (1, 2 * thin), 1)
    qkv_parts = first_half + [jnp.where(lanes < thin, p, 0.0) for p in second]
    proj_parts = [jnp.where(lanes < thin, 0.0, p) for p in second]
    scale_qkv = scale_of(qkv_parts, 3 * thin * thin)
    scale_proj = scale_of(proj_parts, thin * thin)
    for n, i, s, row in spans(one_ref, 0, thin):
        g_qkv_one[row : row + s, 0 : 2 * thin] = (one_ref[n, i : i + s, :] * scale_qkv).astype(bf16)
    for n, i, s, row in spans(one_ref, thin, 2 * thin):
        r = row - thin
        g_qkv_one[r : r + s, 2 * thin : 3 * thin] = (one_ref[n, i : i + s, 0:thin] * scale_qkv).astype(bf16)
        g_proj_one[r : r + s, :] = (one_ref[n, i : i + s, thin : 2 * thin] * scale_proj).astype(bf16)


def shards(
    tokens, cotangent, kinds_one, kinds_two, table_one, table_two, gain_one, gain_merge, gain_two,
    qkv_one, proj_one, merge_weight, qkv_two, proj_two,
):
    c1, c2 = proj_one.shape[0], proj_two.shape[0]
    rows1, cols1 = tokens.shape[1], tokens.shape[2] // c1
    rows2, cols2 = rows1 // 2, cols1 // 2
    nlon, nlat = sizes()
    vmem = pl.BlockSpec(memory_space=pltpu.VMEM)
    stages = place_stages()

    lace1 = lane_rows(rows1, cols1, LEVELS * rows1)
    lace2_pad = rounded_up(LEVELS * rows2, 8)
    lace2 = lane_rows(rows2, cols2, lace2_pad)
    win1, win2 = window_rows(rows1, cols1), window_rows(rows2, cols2)
    group = merge_rows(rows1, cols1)
    ahead = parts_rows(rows1, cols1, True)
    behind = parts_rows(rows1, cols1, False)
    ahead_got = moved(ahead, -HALF_LAT, -HALF_LON, rows1, cols1)
    behind_got = moved(behind, HALF_LAT, HALF_LON, rows1, cols1)
    orders = [
        index_of(win1, lace1),
        index_of(flat(ahead), win1),
        index_of(group, ahead_got),
        index_of(lace2, win2),
        index_of(win2, lace2),
        index_of(flat(behind), group),
        index_of(win1, behind_got),
        index_of(lace1, win1),
    ]
    index = np.full((max(len(o) for o in orders), 128), -1, np.int32)
    for n, order in enumerate(orders):
        index[: len(order), n] = order
    index = jnp.asarray(index)
    sizes_parts = [len(p) for p in ahead]

    lattice = tokens.transpose(1, 0, 2)
    cot = cotangent.transpose(1, 0, 2)
    halos = exchange(*halo_call(lattice, cot, HALF_LON * c1), -1)
    bias_one, bias_two = bias_call(
        kinds_one, kinds_two, table_one.swapaxes(0, 1), table_two.swapaxes(0, 1)
    )

    def part_shapes(dtype=bf16):
        return [jax.ShapeDtypeStruct((n, c1), dtype) for n in sizes_parts]

    def lace_shapes(rows, cols, channels):
        kr, kl, cl = rows - HALF_LAT, (cols - HALF_LON) * channels, HALF_LON * channels
        return [
            jax.ShapeDtypeStruct((r, LEVELS, n), bf16)
            for r, n in ((kr, kl), (HALF_LAT, kl), (kr, cl), (HALF_LAT, cl))
        ]

    count1 = LEVELS * rows1 * cols1
    units1 = count1 // SPOTS
    fwd = pl.pallas_call(
        functools.partial(forward_one_kernel, cols=cols1, columns=(0, 1)),
        name="forward_one",
        in_specs=[vmem] * 9,
        out_specs=[vmem] * 8,
        out_shape=near_out(
            part_shapes()
            + [
                jax.ShapeDtypeStruct((count1, c1), bf16),
                jax.ShapeDtypeStruct((count1, 3 * c1), bf16),
                jax.ShapeDtypeStruct((units1, HEADS1 * SPOTS, 128), bf16),
                jax.ShapeDtypeStruct((count1, c1), bf16),
            ]
        ),
        compiler_params=LIMIT,
        scratch_shapes=[
            pltpu.VMEM((LEVELS * rows1, cols1 * c1), f32),
            pltpu.VMEM((count1, 3 * c1), f32),
            pltpu.VMEM((count1, c1), f32),
        ],
    )(*near_in(lattice, *halos, bias_one, gain_one, qkv_one, proj_one, index))
    parts, kept = fwd[:4], fwd[4:]
    got = exchange(*parts[1:], -1)

    tokens2 = LEVELS * SPOTS
    total_two = 4 * c1 + 4 * c2
    two = pl.pallas_call(
        functools.partial(merge_two_kernel, cols=cols2, columns=(2, 3, 4, 5)),
        name="merge_two",
        in_specs=[vmem] * 15,
        out_specs=[vmem] * 10,
        out_shape=near_out(
            lace_shapes(rows2, cols2, c2)
            + part_shapes()
            + [jax.ShapeDtypeStruct((total_two // 2, c2), bf16)] * 2
        ),
        compiler_params=LIMIT_TWO,
        scratch_shapes=[
            pltpu.VMEM((lace2_pad, cols2 * c2), f32),
            pltpu.VMEM((LEVELS, HEADS2 * SPOTS, 128), f32),
            pltpu.VMEM((tokens2, 3 * c2), f32),
            pltpu.VMEM((tokens2, c2), f32),
            pltpu.VMEM((tokens2, 3 * c2), f32),
            pltpu.VMEM((total_two, c2), f32),
        ],
    )(*near_in(parts[0], *got, cot, *halos, bias_two, gain_merge, gain_two,
                merge_weight, qkv_two, proj_two, index))
    res, d_parts, sums_two = two[:4], two[4:8], two[8:]
    d_got = exchange(*d_parts[1:], 1)
    two_parts = [sums_two[0], pair(sums_two[1])]
    for n in range(len(stages)):
        two_parts = moves(sum_split(two_parts, n), n)

    lanes1, lane1 = tokens.shape[2], HALF_LON * c1
    one = pl.pallas_call(
        functools.partial(backward_one_kernel, cols=cols1, columns=(6, 7)),
        name="backward_one",
        in_specs=[vmem] * 15,
        out_specs=[vmem] * 6,
        out_shape=near_out(
            [
                jax.ShapeDtypeStruct((rows1 - HALF_LAT, LEVELS, lanes1 - lane1), bf16),
                *(jax.ShapeDtypeStruct(h.shape, bf16) for h in halos),
            ]
            + [jax.ShapeDtypeStruct((c1, 2 * c1), bf16)] * 2
        ),
        compiler_params=LIMIT,
        scratch_shapes=[
            pltpu.VMEM((LEVELS * rows1, cols1 * c1), f32),
            pltpu.VMEM((count1, 3 * c1), f32),
            pltpu.VMEM((count1, c1), f32),
            pltpu.VMEM((count1, 3 * c1), f32),
            pltpu.VMEM((c1, 4 * c1), f32),
        ],
    )(*near_in(d_parts[0], *d_got, *kept, *res[1:], gain_one, qkv_one, proj_one, index))
    d_tok, sums_one = one[:4], one[4:]
    one_parts = [sums_one[0], pair(sums_one[1])]
    one_parts = moves(sum_split(one_parts, 0), 0)
    message = message_of(two_parts, one_parts)
    small = one_parts[0].shape[0]
    for n in range(len(stages) - 1, 0, -1):
        message = widen(moves([message] * stages[n][0], n), small)
    own = moves([message] * stages[0][0], 0)
    far = [pair(m) for m in own]
    back = exchange(*d_tok[1:], 1)
    joined = pl.pallas_call(
        join_kernel,
        name="join",
        in_specs=[vmem] * 5,
        out_specs=[vmem] * 2,
        out_shape=[
            jax.ShapeDtypeStruct((rows2, LEVELS, lanes1), bf16),
            jax.ShapeDtypeStruct((rows1, LEVELS, lanes1), bf16),
        ],
        compiler_params=LIMIT,
    )(*near_in(res[0], d_tok[0], *back))
    result, d_tokens = (v.transpose(1, 0, 2) for v in joined)

    near = stages[0][0]
    inner = 1
    for size, _, _ in stages[1:]:
        inner *= size
    grads = pl.pallas_call(
        functools.partial(finish_kernel, stage_sizes=tuple(size for size, _, _ in stages)),
        name="finish",
        in_specs=[vmem] * (2 * near),
        out_specs=[vmem] * 5,
        out_shape=[
            jax.ShapeDtypeStruct(w.shape, bf16) for w in (qkv_one, proj_one, merge_weight, qkv_two, proj_two)
        ],
        scratch_shapes=[
            pltpu.VMEM((2 * near * inner,) + two_parts[0].shape, f32),
            pltpu.VMEM((2 * near,) + one_parts[0].shape, f32),
        ],
        compiler_params=LIMIT,
    )(*near_in(*own, *far))
    return (result, d_tokens, *grads)


def solution(mesh):
    tiled = P(None, "lat", "lon")
    in_specs = (tiled, tiled, P(None, "lat"), P(None, "lat")) + (P(),) * 10
    out_specs = (tiled, tiled, P(), P(), P(), P(), P())

    return jax.shard_map(shards, mesh=mesh, in_specs=in_specs, out_specs=out_specs, check_vma=False)
```

```python
import functools

import jax
import jax.numpy as jnp
import numpy as np
from jax import lax
from jax.experimental import pallas as pl
from jax.experimental.pallas import tpu as pltpu
from jax.sharding import PartitionSpec as P


HEADS1 = 6
HEADS2 = 12
HEAD = 32
WIN_LAT = 6
WIN_LON = 12
HALF_LAT = WIN_LAT // 2
HALF_LON = WIN_LON // 2
SPOTS = WIN_LAT * WIN_LON
SPAN = 2 * WIN_LON - 1
LEVELS = 2

BATCH = (1, 3, 6, 8)

norm_epsilon = 1e-05
grad_epsilon = 1e-06
masked_score = -1e30

f32 = jnp.float32
bf16 = jnp.bfloat16
AXES = ("lon", "lat")


def rounded_up(count, step):
    return -(-count // step) * step


def core_of():
    return lax.axis_index("lon") % 2


def mm(a, b):
    return lax.dot_general(a, b, (((1,), (0,)), ((), ())), preferred_element_type=f32)


def mm_nt(a, b):
    return lax.dot_general(a, b, (((1,), (1,)), ((), ())), preferred_element_type=f32)


def mm_tn(a, b):
    return lax.dot_general(a, b, (((0,), (0,)), ((), ())), preferred_element_type=f32)


LIMIT = pltpu.CompilerParams(vmem_limit_bytes=24 << 20)

LIMIT_TWO = pltpu.CompilerParams(vmem_limit_bytes=24 << 20)


def near_in(*values):
    return [pltpu.with_memory_space_constraint(v, pltpu.VMEM) for v in values]


def far_in(*values):
    return [pltpu.with_memory_space_constraint(v, pltpu.HBM) for v in values]


def near_out(shapes):
    return [pltpu.VMEM(s.shape, s.dtype) for s in shapes]


def parts_rows(rows, cols, ahead):
    keep_r, keep_c = rows - HALF_LAT, cols - HALF_LON
    if ahead:
        row_sets = (range(HALF_LAT, rows), range(HALF_LAT))
        col_sets = (range(HALF_LON, cols), range(HALF_LON))
    else:
        row_sets = (range(keep_r), range(keep_r, rows))
        col_sets = (range(keep_c), range(keep_c, cols))
    out = []
    for rset, cset in ((0, 0), (1, 0), (0, 1), (1, 1)):
        piece = [(z, j, k) for z in range(LEVELS) for j in row_sets[rset] for k in col_sets[cset]]
        piece += [None] * (rounded_up(len(piece), 16) - len(piece))
        out.append(piece)
    return out


def window_rows(rows, cols):
    return [
        (z, b * WIN_LAT + ap, c * WIN_LON + bp)
        for b in range(rows // WIN_LAT)
        for c in range(cols // WIN_LON)
        for z in range(LEVELS)
        for ap in range(WIN_LAT)
        for bp in range(WIN_LON)
    ]


def merge_rows(rows, cols):
    return [
        (z, 2 * jj + a, 2 * kk + b)
        for a in range(2)
        for b in range(2)
        for z in range(LEVELS)
        for jj in range(rows // 2)
        for kk in range(cols // 2)
    ]


def lane_rows(rows, cols, pad):
    out = []
    for k in range(cols):
        group = [(1 - z, j, k) for j in range(rows) for z in range(LEVELS)]
        out += group + [None] * (pad - len(group))
    return out


def index_of(wanted, source):
    where = {spot: n for n, spot in enumerate(source) if spot is not None}
    return [-1 if spot is None else where[spot] for spot in wanted]


def flat(pieces):
    return [spot for piece in pieces for spot in piece]


def moved(pieces, dj, dk, rows, cols):
    return [
        None if s is None else (s[0], (s[1] + dj) % rows, (s[2] + dk) % cols) for s in flat(pieces)
    ]


def one_hot(index_ref, column, count, width):
    index = index_ref[0:count, column : column + 1]
    lanes = lax.broadcasted_iota(jnp.int32, (count, width), 1)
    return jnp.where(index == lanes, 1.0, 0.0).astype(bf16)


def lane_head_masks(width):
    lanes = lax.broadcasted_iota(jnp.int32, (1, width), 1)
    return [
        jnp.where((lanes >= h * HEAD) & (lanes < (h + 1) * HEAD), 1.0, 0.0).astype(f32)
        for h in range(width // HEAD)
    ]


def spread_heads(values, masks):
    return jnp.concatenate([values * m for m in masks], axis=0)


def gather_heads(stack, masks):
    total = stack[0:SPOTS] * masks[0]
    for h in range(1, len(masks)):
        total = total + stack[h * SPOTS : (h + 1) * SPOTS] * masks[h]
    return total


def head_groups(channels):
    out = []
    at = 0
    while at < channels:
        width = min(128, channels - at)
        out.append((at, width))
        at += width
    return out


def rms_stats(values):
    centre = jnp.mean(values, axis=-1, keepdims=True)
    spread = values - centre
    second = jnp.mean(spread * spread, axis=-1, keepdims=True)
    scale = lax.rsqrt(second + norm_epsilon)
    return spread * scale, scale


def norm_back(hat, scale, d_hat, count):
    first = jnp.sum(d_hat, axis=-1, keepdims=True) * (1.0 / count)
    second = jnp.sum(d_hat * hat, axis=-1, keepdims=True) * (1.0 / count)
    return scale * (d_hat - first - hat * second)


def softmax_rows(scores):
    top = jnp.max(scores, axis=-1, keepdims=True)
    weights = jnp.exp(scores - top)
    return weights / jnp.sum(weights, axis=-1, keepdims=True)


def halo_kernel(tokens, cot, lat, lon, diag, sems):
    copies = halo_copies(tokens, cot, lat, lon, diag, sems)
    for c in copies:
        c.start()
    for c in copies:
        c.wait()


def expand_bias(kinds_one, kinds_two, table_one, table_two, target, out_one, out_two, rows_ref, runs_ref):
    bands = out_one.shape[0] // LEVELS
    head_sets = [(8 * b, HEADS1) for b in range(bands)] + [(8 * bands, HEADS2)]
    width = WIN_LAT * SPAN
    slots = rows_ref.shape[0]
    rows_ref[...] = jnp.zeros(rows_ref.shape, f32)
    for b in range(bands):
        for h in range(HEADS1):
            rows_ref[8 * b + h : 8 * b + h + 1, :] = table_one[h, pl.ds(kinds_one[0, b], 1), :]
    for h in range(HEADS2):
        at = 8 * bands + h
        rows_ref[at : at + 1, :] = table_two[h, pl.ds(kinds_two[0, 0], 1), :]
    runs_ref[...] = jnp.zeros(runs_ref.shape, f32)
    for z in range(LEVELS):
        for ap in range(WIN_LAT):
            start = (z * (LEVELS + 1)) * WIN_LAT * width + ap * width
            at = (z * WIN_LAT + ap) * slots
            runs_ref[at : at + slots, 0:width] = rows_ref[:, start : start + width]
    runs = runs_ref[...]
    high = runs.astype(bf16)
    rest = runs - high.astype(f32)
    middle = rest.astype(bf16)
    low = (rest - middle.astype(f32)).astype(bf16)
    sub = lax.broadcasted_iota(jnp.int32, (256, target.shape[1]), 0)
    pick = jnp.where(sub == target[0:1, :], 1.0, 0.0).astype(bf16)
    full = mm(high, pick) + mm(middle, pick) + mm(low, pick)
    lanes = lax.broadcasted_iota(jnp.int32, (1, 128), 1)
    at_end = jnp.where(lax.axis_index("lat") == lax.axis_size("lat") - 1, 1.0, 0.0).astype(f32)
    for z in range(LEVELS):
        for ap in range(WIN_LAT):
            across = jnp.where(
                (lanes >= SPOTS // 2) if ap < HALF_LAT else (lanes < SPOTS // 2), masked_score, 0.0
            )
            at = (z * WIN_LAT + ap) * slots
            for s, (first, heads) in enumerate(head_sets):
                own = across * at_end if s >= bands - 1 else jnp.zeros_like(across)
                for bp in range(WIN_LON):
                    piece = full[at + first : at + first + heads, 128 * bp : 128 * bp + 128] + own
                    spot = ap * WIN_LON + bp
                    if s < bands:
                        out_one[s * LEVELS + z, pl.ds(spot, heads, stride=SPOTS), :] = piece
                    else:
                        out_two[z, pl.ds(spot, heads, stride=SPOTS), :] = piece


def bias_call(kinds_one, kinds_two, table_one, table_two):
    bands = kinds_one.shape[1]
    target = np.full((8, WIN_LON * 128), -1, np.int32)
    for bp in range(WIN_LON):
        for aq in range(WIN_LAT):
            for bq in range(WIN_LON):
                target[:, bp * 128 + aq * WIN_LON + bq] = aq * SPAN + bp - bq + WIN_LON - 1
    slots = 8 * bands + rounded_up(HEADS2, 8)
    smem = pl.BlockSpec(memory_space=pltpu.SMEM)
    vmem = pl.BlockSpec(memory_space=pltpu.VMEM)
    return pl.pallas_call(
        expand_bias,
        name="bias",
        in_specs=[smem, smem, vmem, vmem, vmem],
        out_specs=[vmem] * 2,
        out_shape=(
            pltpu.VMEM((bands * LEVELS, HEADS1 * SPOTS, 128), f32),
            pltpu.VMEM((LEVELS, HEADS2 * SPOTS, 128), f32),
        ),
        compiler_params=LIMIT,
        scratch_shapes=[
            pltpu.VMEM((slots, table_one.shape[2]), f32),
            pltpu.VMEM((LEVELS * WIN_LAT * slots, 256), f32),
        ],
    )(kinds_one, kinds_two, *far_in(table_one, table_two, jnp.asarray(target)))


def halo_call(tokens, cot, lane1):
    rows, levels, lanes = tokens.shape
    low = cot.shape[0] - HALF_LAT
    return pl.pallas_call(
        halo_kernel,
        name="halo",
        in_specs=[pl.BlockSpec(memory_space=pl.ANY)] * 2,
        out_specs=[pl.BlockSpec(memory_space=pltpu.VMEM)] * 3,
        out_shape=(
            pltpu.VMEM((HALF_LAT, levels, 2 * lanes - 3 * lane1), bf16),
            pltpu.VMEM((rows - HALF_LAT + 2 * low, levels, lane1), bf16),
            pltpu.VMEM((HALF_LAT, levels, 3 * lane1), bf16),
        ),
        compiler_params=LIMIT,
        scratch_shapes=[pltpu.SemaphoreType.DMA((7,))],
    )(*far_in(tokens, cot))


def halo_copies(tokens, cot, lat, lon, diag, sems):
    rows, lanes = tokens.shape[0], tokens.shape[2]
    cut = HALF_LAT
    lane1 = diag.shape[2] // 3
    lane2 = 2 * lane1
    kept1 = lanes - lane1
    jobs = [
        (tokens.at[0:cut, :, lane1:lanes], lat.at[:, :, 0:kept1]),
        (cot.at[0:cut, :, lane2:lanes], lat.at[:, :, kept1 : kept1 + lanes - lane2]),
        (tokens.at[cut:rows, :, 0:lane1], lon.at[0 : rows - cut]),
        (tokens.at[0:cut, :, 0:lane1], diag.at[:, :, 0:lane1]),
        (cot.at[0:cut, :, 0:lane2], diag.at[:, :, lane1 : lane1 + lane2]),
    ]
    low = cot.shape[0] - cut
    for n in range(2):
        at = rows - cut + n * low
        jobs.append((cot.at[cut : cut + low, :, n * lane1 : (n + 1) * lane1], lon.at[at : at + low]))
    return [pltpu.make_async_copy(a, b, sems.at[n]) for n, (a, b) in enumerate(jobs)]


def unlace_one(main, lat, lon, diag, lace_ref, lane1):
    rows, lanes = main.shape[0], main.shape[2]
    kept = lanes - lane1
    for j in range(rows - HALF_LAT):
        lace_ref[2 * j : 2 * j + 2, 0:kept] = main[j + HALF_LAT, :, lane1:lanes].astype(f32)
        lace_ref[2 * j : 2 * j + 2, kept:lanes] = lon[j].astype(f32)
    for n in range(HALF_LAT):
        j = rows - HALF_LAT + n
        lace_ref[2 * j : 2 * j + 2, 0:kept] = lat[n, :, 0:kept].astype(f32)
        lace_ref[2 * j : 2 * j + 2, kept:lanes] = diag[n, :, 0:lane1].astype(f32)


def unlace_two(main, lat, lon, diag, lace_ref, lane1):
    rows, lanes = main.shape[0], main.shape[2]
    lane2 = 2 * lane1
    kept = lanes - lane2
    low = rows - HALF_LAT
    first = lon.shape[0] - 2 * low
    for j in range(low):
        lace_ref[2 * j : 2 * j + 2, 0:kept] = main[j + HALF_LAT, :, lane2:lanes].astype(f32)
        for n in range(2):
            at = kept + n * lane1
            lace_ref[2 * j : 2 * j + 2, at : at + lane1] = lon[first + n * low + j].astype(f32)
    for n in range(HALF_LAT):
        j = low + n
        lace_ref[2 * j : 2 * j + 2, 0:kept] = lat[n, :, lanes - lane1 : lanes - lane1 + kept].astype(f32)
        lace_ref[2 * j : 2 * j + 2, kept:lanes] = diag[n, :, lane1 : lane1 + lane2].astype(f32)


def lace_out(lace_ref, main, lat, lon, diag, cut_row, cut_lane):
    rows = main.shape[0] + cut_row
    kept = main.shape[2]
    lanes = kept + cut_lane
    for j in range(rows - cut_row):
        main[j] = lace_ref[2 * j : 2 * j + 2, 0:kept].astype(bf16)
        lon[j] = lace_ref[2 * j : 2 * j + 2, kept:lanes].astype(bf16)
    for n in range(cut_row):
        j = rows - cut_row + n
        lat[n] = lace_ref[2 * j : 2 * j + 2, 0:kept].astype(bf16)
        diag[n] = lace_ref[2 * j : 2 * j + 2, kept:lanes].astype(bf16)


def forward_one_kernel(
    main, lat, lon, diag, bias, gain, w_qkv, w_proj, index,
    out_main, out_lat, out_lon, out_diag, keep_x, keep_packed, keep_probs, keep_att,
    lace_ref, packed_ref, att_ref,
    *, cols, columns,
):
    channels = gain.shape[0]
    lace_rows = lace_ref.shape[0]
    count = lace_rows * cols
    unlace_one(main, lat, lon, diag, lace_ref, HALF_LON * channels)
    stacked = jnp.concatenate(
        [lace_ref[:, channels * k : channels * (k + 1)] for k in range(cols)], axis=0
    ).astype(bf16)
    values = mm(one_hot(index, columns[0], count, count), stacked)
    hat, _ = rms_stats(values)
    normed = (hat * gain[...][None, :]).astype(bf16)
    packed = mm(normed, w_qkv[...]).astype(bf16)
    packed_ref[...] = packed.astype(f32)
    keep_packed[...] = packed
    keep_x[...] = values.astype(bf16)
    units = count // SPOTS
    bands_span = bias.shape[0] // LEVELS
    per_band = units // bands_span

    def bias_of(key_of):
        u, rows = key_of
        return bias[u // per_band * LEVELS + u % LEVELS, rows, 0:SPOTS]

    def keep(key_of, weights):
        u, rows = key_of
        keep_probs[u, rows, 0:SPOTS] = weights.astype(bf16)

    attention(packed_ref, att_ref, bias_of, keep, head_jobs(units, channels), channels, BATCH[0])
    attended = att_ref[...].astype(bf16)
    keep_att[...] = attended
    block = (values + mm(attended, w_proj[...])).astype(bf16)
    start = 0
    total = out_main.shape[0] + out_lat.shape[0] + out_lon.shape[0] + out_diag.shape[0]
    parts = mm(one_hot(index, columns[1], total, count), block).astype(bf16)
    for out in (out_main, out_lat, out_lon, out_diag):
        out[...] = parts[start : start + out.shape[0]]
        start += out.shape[0]


def cotangent_kernel(main, lat, lon, diag, w_proj, index, d_block, d_att, lace_ref, *, thin, cols, column):
    channels = w_proj.shape[0]
    tokens = d_block.shape[0]
    lace_rows = lace_ref.shape[0]
    lace_ref[...] = jnp.zeros(lace_ref.shape, f32)
    unlace_two(main, lat, lon, diag, lace_ref, HALF_LON * thin)
    stack = jnp.concatenate(
        [lace_ref[:, channels * k : channels * (k + 1)] for k in range(cols)], axis=0
    ).astype(bf16)
    rolled = mm(one_hot(index, column, tokens, lace_rows * cols), stack).astype(bf16)
    d_block[...] = rolled
    d_att[...] = mm_nt(rolled, w_proj[...]).astype(bf16).astype(f32)


def merge_two_kernel(
    main, lat, lon, diag, d_block_in, d_att_in, bias,
    gain_merge, gain_two, w_merge, w_qkv, w_proj, index,
    out_block, d_main, d_lat, d_lon, d_diag, sums_keep, sums_send,
    probs_ref, packed_ref, att_ref, d_packed_ref, sums_ref,
    *, columns,
):
    channels = gain_two.shape[0]
    thin = main.shape[1]
    groups = gain_merge.shape[0] // thin
    tokens = LEVELS * SPOTS
    total = main.shape[0] + lat.shape[0] + lon.shape[0] + diag.shape[0]
    stacked = jnp.concatenate([main[...], lat[...], lon[...], diag[...]], axis=0)
    grouped = mm(one_hot(index, columns[0], groups * tokens, total), stacked)
    pieces = [grouped[g * tokens : (g + 1) * tokens] for g in range(groups)]
    wide = groups * thin
    centre = sum(jnp.sum(p, axis=-1, keepdims=True) for p in pieces) * (1.0 / wide)
    spreads = [p - centre for p in pieces]
    second = sum(jnp.sum(s * s, axis=-1, keepdims=True) for s in spreads) * (1.0 / wide)
    scale_merge = lax.rsqrt(second + norm_epsilon)
    hats = [s * scale_merge for s in spreads]
    wide_gain = gain_merge[...][None, :]
    gains = [wide_gain[:, g * thin : (g + 1) * thin] for g in range(groups)]
    merged_norm = [(hats[g] * gains[g]).astype(bf16) for g in range(groups)]
    merged = mm(merged_norm[0], w_merge[0:thin, :])
    for g in range(1, groups):
        merged = merged + mm(merged_norm[g], w_merge[g * thin : (g + 1) * thin, :])
    merged = merged.astype(bf16).astype(f32)
    hat, scale_two = rms_stats(merged)
    normed = (hat * gain_two[...][None, :]).astype(bf16)
    packed_ref[...] = mm(normed, w_qkv[...]).astype(bf16).astype(f32)

    def keep(key_of, weights):
        probs_ref[key_of[0], key_of[1], 0:SPOTS] = weights

    jobs = head_jobs(LEVELS, channels)
    attention(
        packed_ref, att_ref, lambda k: bias[k[0], k[1], 0:SPOTS], keep, jobs, channels, BATCH[1]
    )
    attended = att_ref[...].astype(bf16)
    block = (merged + mm(attended, w_proj[...])).astype(bf16)
    out_block[...] = block
    d_block_low = d_block_in[...]
    d_block = d_block_low.astype(f32)
    at_sum = groups * thin
    sums_ref[at_sum : at_sum + channels, :] = mm_tn(attended, d_block_low)
    attention_back(
        packed_ref, d_att_in, d_packed_ref, lambda k: probs_ref[k[0], k[1], 0:SPOTS], jobs, channels, BATCH[2]
    )
    d_packed = d_packed_ref[...].astype(bf16)
    at_sum += channels
    for n in range(3):
        sums_ref[at_sum + n * channels : at_sum + (n + 1) * channels, :] = mm_tn(
            normed, d_packed[:, n * channels : (n + 1) * channels]
        )
    d_normed = mm_nt(d_packed, w_qkv[...]).astype(bf16).astype(f32)
    d_merged = d_block + norm_back(hat, scale_two, d_normed * gain_two[...][None, :], channels)
    d_merged = d_merged.astype(bf16)
    d_hats = []
    for g in range(groups):
        sums_ref[g * thin : (g + 1) * thin, :] = mm_tn(merged_norm[g], d_merged)
        d_norm = mm_nt(d_merged, w_merge[g * thin : (g + 1) * thin, :]).astype(bf16).astype(f32)
        d_hats.append(d_norm * gains[g])
    first = sum(jnp.sum(d, axis=-1, keepdims=True) for d in d_hats) * (1.0 / wide)
    cross = sum(jnp.sum(d * h, axis=-1, keepdims=True) for d, h in zip(d_hats, hats)) * (1.0 / wide)
    d_group = jnp.concatenate(
        [scale_merge * (d_hats[g] - first - hats[g] * cross) for g in range(groups)], axis=0
    ).astype(bf16)
    parts = mm(one_hot(index, columns[1], total, groups * tokens), d_group).astype(bf16)
    start = 0
    for out in (d_main, d_lat, d_lon, d_diag):
        out[...] = parts[start : start + out.shape[0]]
        start += out.shape[0]
    half = sums_ref.shape[0] // 2
    mine = core_of()
    first_row = pl.multiple_of(mine * half, 16)
    other_row = pl.multiple_of((1 - mine) * half, 16)
    sums_keep[...] = sums_ref[pl.ds(first_row, half), :].astype(bf16)
    sums_send[...] = sums_ref[pl.ds(other_row, half), :].astype(bf16)


def qkv_of(packed_ref, r0, at, width, channels):
    rows = slice(r0, r0 + SPOTS)
    query = packed_ref[rows, at : at + width]
    key = packed_ref[rows, channels + at : channels + at + width].astype(bf16)
    value = packed_ref[rows, 2 * channels + at : 2 * channels + at + width].astype(bf16)
    return query, key, value


def batches(jobs, size):
    return [jobs[n : n + size] for n in range(0, len(jobs), size)]


def attention_back(packed_ref, d_att_ref, d_packed_ref, probs_of, jobs, channels, size):
    for batch in batches(jobs, size):
        state = []
        for r0, at, width, key_of in batch:
            masks = lane_head_masks(width)
            value = qkv_of(packed_ref, r0, at, width, channels)[2]
            d_att = spread_heads(d_att_ref[r0 : r0 + SPOTS, at : at + width], masks).astype(bf16)
            state.append((d_att, mm_nt(d_att, value)))
        scores = []
        for (r0, at, width, key_of), (d_att, d_probs) in zip(batch, state):
            probs = probs_of(key_of).astype(f32)
            d_probs = d_probs.astype(bf16).astype(f32)
            inner = jnp.sum(probs * d_probs, axis=-1, keepdims=True)
            scores.append((probs * (d_probs - inner) * HEAD ** (-0.5)).astype(bf16))
        for (r0, at, width, key_of), (d_att, _), d_scores in zip(batch, state, scores):
            masks = lane_head_masks(width)
            query, key, _ = qkv_of(packed_ref, r0, at, width, channels)
            rows = slice(r0, r0 + SPOTS)
            d_packed_ref[rows, at : at + width] = gather_heads(mm(d_scores, key), masks)
            d_packed_ref[rows, channels + at : channels + at + width] = mm_tn(
                d_scores, spread_heads(query, masks).astype(bf16)
            )
            d_packed_ref[rows, 2 * channels + at : 2 * channels + at + width] = mm_tn(
                probs_of(key_of).astype(bf16), d_att
            )


def attention(packed_ref, att_ref, bias_of, keep, jobs, channels, size):
    for batch in batches(jobs, size):
        scores = []
        for r0, at, width, key_of in batch:
            masks = lane_head_masks(width)
            query, key, _ = qkv_of(packed_ref, r0, at, width, channels)
            scores.append(mm_nt(spread_heads(query, masks).astype(bf16), key))
        probs = []
        for (r0, at, width, key_of), score in zip(batch, scores):
            weights = softmax_rows(score * HEAD ** (-0.5) + bias_of(key_of))
            keep(key_of, weights)
            probs.append(weights.astype(bf16))
        for (r0, at, width, key_of), weights in zip(batch, probs):
            value = qkv_of(packed_ref, r0, at, width, channels)[2]
            att_ref[r0 : r0 + SPOTS, at : at + width] = gather_heads(
                mm(weights, value), lane_head_masks(width)
            )


def head_jobs(units, channels):
    return [
        (u * SPOTS, at, width, (u, slice(at // HEAD * SPOTS, (at + width) // HEAD * SPOTS)))
        for u in range(units)
        for at, width in head_groups(channels)
    ]


def backward_one_kernel(
    main, lat, lon, diag, keep_x, keep_packed, keep_probs, keep_att, block_two,
    gain, w_qkv, w_proj, index,
    res_main, out_main, out_lat, out_lon, out_diag, sums_keep, sums_send,
    lace_ref, packed_ref, att_ref, d_packed_ref, sums_ref, lace_two_ref,
    *, cols, columns,
):
    channels = gain.shape[0]
    lace_rows = lace_ref.shape[0]
    count = lace_rows * cols
    total = main.shape[0] + lat.shape[0] + lon.shape[0] + diag.shape[0]
    stacked = jnp.concatenate([main[...], lat[...], lon[...], diag[...]], axis=0)
    d_block = mm(one_hot(index, columns[0], count, total), stacked)
    d_block_low = d_block.astype(bf16)
    hat, scale = rms_stats(keep_x[...].astype(f32))
    normed = (hat * gain[...][None, :]).astype(bf16)
    packed_ref[...] = keep_packed[...].astype(f32)
    att_ref[...] = mm_nt(d_block_low, w_proj[...]).astype(bf16).astype(f32)
    attention_back(
        packed_ref, att_ref, d_packed_ref, lambda k: keep_probs[k[0], k[1], 0:SPOTS],
        head_jobs(count // SPOTS, channels), channels, BATCH[3],
    )
    d_packed = d_packed_ref[...].astype(bf16)
    sums_ref[:, 0 : 3 * channels] = mm_tn(normed, d_packed)
    sums_ref[:, 3 * channels : 4 * channels] = mm_tn(keep_att[...], d_block_low)
    d_normed = mm_nt(d_packed, w_qkv[...]).astype(bf16).astype(f32)
    d_shift = d_block + norm_back(hat, scale, d_normed * gain[...][None, :], channels)
    lattice = mm(one_hot(index, columns[1], count, count), d_shift.astype(bf16))
    for k in range(cols):
        lace_ref[:, channels * k : channels * (k + 1)] = lattice[lace_rows * k : lace_rows * (k + 1)]
    kept = out_main.shape[2]
    lane1 = HALF_LON * channels
    low = out_main.shape[0]
    lace_out(
        lace_ref, out_main, out_lat.at[:, :, 0:kept], out_lon.at[0:low], out_diag.at[:, :, 0:lane1],
        HALF_LAT, lane1,
    )
    wide = block_two.shape[1]
    wide_rows = lace_two_ref.shape[0]
    wide_cols = lace_two_ref.shape[1] // wide
    lattice = mm(
        one_hot(index, columns[2], wide_rows * wide_cols, block_two.shape[0]), block_two[...]
    )
    for k in range(wide_cols):
        lace_two_ref[:, wide * k : wide * (k + 1)] = lattice[wide_rows * k : wide_rows * (k + 1)]
    kept_two = res_main.shape[2]
    lanes = lace_two_ref.shape[1]
    count = res_main.shape[0]
    for j in range(count):
        row = lace_two_ref[2 * j : 2 * j + 2, :].astype(bf16)
        res_main[j] = row[:, 0:kept_two]
        for n in range(2):
            at = kept_two + n * lane1
            out_lon[low + n * count + j] = row[:, at : at + lane1]
    for n in range(HALF_LAT):
        at = 2 * (count + n)
        row = lace_two_ref[at : at + 2, :].astype(bf16)
        out_lat[n, :, kept : kept + kept_two] = row[:, 0:kept_two]
        out_diag[n, :, lane1 : lane1 + lanes - kept_two] = row[:, kept_two:lanes]
    mine = core_of()
    half = 2 * channels
    low = sums_ref[:, 0:half].astype(bf16)
    high = sums_ref[:, half : 2 * half].astype(bf16)

    @pl.when(mine == 0)
    def _():
        sums_keep[...] = low
        sums_send[...] = high

    @pl.when(mine != 0)
    def _():
        sums_keep[...] = high
        sums_send[...] = low


def sizes():
    return lax.axis_size("lon"), lax.axis_size("lat")


def send(values, lon_step, lat_step):
    nlon, nlat = sizes()
    route = [
        (i * nlat + j, ((i + lon_step) % nlon) * nlat + (j + lat_step) % nlat)
        for i in range(nlon)
        for j in range(nlat)
    ]
    return lax.ppermute(values, AXES, route)


def exchange(lat, lon, diag, step):
    return (send(lat, 0, step), send(lon, step, 0), send(diag, step, step))


def join_kernel(res_main, d_main, lat, lon, diag, result, d_tokens):
    rows, lanes = d_tokens.shape[0], d_tokens.shape[2]
    cut = HALF_LAT
    kept = d_main.shape[2]
    lane1 = lanes - kept
    d_tokens[cut:rows, :, lane1:lanes] = d_main[...]
    d_tokens[0:cut, :, lane1:lanes] = lat[:, :, 0:kept]
    d_tokens[cut:rows, :, 0:lane1] = lon[0 : rows - cut]
    d_tokens[0:cut, :, 0:lane1] = diag[:, :, 0:lane1]
    low = res_main.shape[0]
    lane2 = 2 * lane1
    result[cut : cut + low, :, lane2:lanes] = res_main[...]
    result[0:cut, :, lane2:lanes] = lat[:, :, kept:]
    result[0:cut, :, 0:lane2] = diag[:, :, lane1:]
    for n in range(2):
        at = rows - cut + n * low
        result[cut : cut + low, :, n * lane1 : (n + 1) * lane1] = lon[at : at + low]


def place_stages():
    nlon, nlat = sizes()
    near_lon = 2 if nlon % 4 == 0 else 1
    near_lat = 2 if nlat % 2 == 0 else 1
    far_lon = nlon // 2 // near_lon
    far_lat = nlat // near_lat

    def near(i, j, d):
        c, x, z = i % 2, i // 2 % near_lon, i // 2 // near_lon
        y, w = j % near_lat, j // near_lat
        place = (x * near_lat + y) ^ d
        return (z * near_lon + place // near_lat) * 2 + c, w * near_lat + place % near_lat

    def wide(i, j, d):
        z = i // 2 // near_lon
        return target(z, d, far_lon) * 2 * near_lon + i % (2 * near_lon), j

    def high(i, j, d):
        return i, target(j // near_lat, d, far_lat) * near_lat + j % near_lat

    lon_at, lat_at = lax.axis_index("lon"), lax.axis_index("lat")
    near_at = (lon_at // 2 % near_lon) * near_lat + lat_at % near_lat
    stages = [(near_lon * near_lat, near, near_at)]
    if far_lon > 1:
        stages.append((far_lon, wide, lon_at // 2 // near_lon))
    if far_lat > 1:
        stages.append((far_lat, high, lat_at // near_lat))
    return stages


def hop(values, step, d):
    nlon, nlat = sizes()
    route = []
    for i in range(nlon):
        for j in range(nlat):
            to_lon, to_lat = step(i, j, d)
            route.append((i * nlat + j, to_lon * nlat + to_lat))
    return lax.ppermute(values, AXES, route)


def pair(values):
    return hop(values, lambda i, j, d: (i ^ 1, j), 1)


def near_target(at, d, size):
    return at ^ d


def target(at, d, size):
    return (at + d) % size


def source(at, d, size):
    return lax.rem(at - d + size, size)


def total_of(refs, rows):
    total = refs[0][rows, :].astype(f32)
    for r in refs[1:]:
        total = total + r[rows, :].astype(f32)
    return total


def split_kernel(*refs, count, stage):
    size, _, at = place_stages()[stage]
    outs, scratch = refs[count:-1], refs[-1]
    rows = scratch.shape[1]
    for p in range(size):
        scratch[p] = total_of(refs[:count], slice(p * rows, (p + 1) * rows))
    for d in range(size):
        outs[d][...] = scratch[(near_target if stage == 0 else target)(at, d, size)].astype(bf16)


def sum_split(values, stage):
    size = place_stages()[stage][0]
    rows, width = values[0].shape
    vmem = pl.BlockSpec(memory_space=pltpu.VMEM)
    return pl.pallas_call(
        functools.partial(split_kernel, count=len(values), stage=stage),
        in_specs=[vmem] * len(values),
        out_specs=[vmem] * size,
        out_shape=[pltpu.VMEM((rows // size, width), bf16)] * size,
        scratch_shapes=[pltpu.VMEM((size, rows // size, width), f32)],
        compiler_params=LIMIT,
    )(*near_in(*values))


def message_kernel(*refs, count):
    out = refs[-1]
    rows = refs[0].shape[0]
    out[0:rows, :] = total_of(refs[:count], slice(0, rows)).astype(bf16)
    small = refs[count].shape[0]
    out[rows : rows + small, :] = total_of(refs[count:-1], slice(0, small)).astype(bf16)


def message_of(two, one):
    vmem = pl.BlockSpec(memory_space=pltpu.VMEM)
    values = [*two, *one]
    return pl.pallas_call(
        functools.partial(message_kernel, count=len(two)),
        name="message",
        in_specs=[vmem] * len(values),
        out_specs=vmem,
        out_shape=pltpu.VMEM((two[0].shape[0] + one[0].shape[0], two[0].shape[1]), bf16),
        compiler_params=LIMIT,
    )(*near_in(*values))


def widen_kernel(*refs, rows):
    out, ins = refs[-1], refs[:-1]
    for n, r in enumerate(ins):
        out[n * rows : (n + 1) * rows, :] = r[0:rows, :]
    total = ins[0].shape[0]
    out[len(ins) * rows :, :] = total_of(ins, slice(rows, total)).astype(bf16)


def widen(messages, small):
    vmem = pl.BlockSpec(memory_space=pltpu.VMEM)
    rows = messages[0].shape[0] - small
    return pl.pallas_call(
        functools.partial(widen_kernel, rows=rows),
        name="widen",
        in_specs=[vmem] * len(messages),
        out_specs=vmem,
        out_shape=pltpu.VMEM((rows * len(messages) + small, messages[0].shape[1]), bf16),
        compiler_params=LIMIT,
    )(*near_in(*messages))


def moves(values, stage):
    size, step, _ = place_stages()[stage]
    return [values[0]] + [hop(values[d], step, d) for d in range(1, size)]


def finish_kernel(*refs, stage_sizes):
    near = stage_sizes[0]
    own, far = refs[:near], refs[near : 2 * near]
    g_qkv_one, g_proj_one, g_merge, g_qkv_two, g_proj_two, two_ref, one_ref = refs[2 * near :]
    mine = core_of()
    spots = [at for _, _, at in place_stages()]
    inner = two_ref.shape[0] // (2 * near)
    size = two_ref.shape[1]
    places = [jnp.int32(0)]
    width = 1
    for n in range(len(stage_sizes) - 1, 0, -1):
        count = stage_sizes[n]
        places = [source(spots[n], d, count) * width + p for d in range(count) for p in places]
        width *= count
    for d in range(near):
        place = spots[0] ^ d
        for p in range(inner):
            rows = slice(p * size, (p + 1) * size)
            at = place * inner + places[p]
            two_ref[mine * near * inner + at] = own[d][rows, :].astype(f32)
            two_ref[(1 - mine) * near * inner + at] = far[d][rows, :].astype(f32)
        rows = slice(inner * size, own[d].shape[0])
        one_ref[mine * near + place] = own[d][rows, :].astype(f32)
        one_ref[(1 - mine) * near + place] = far[d][rows, :].astype(f32)

    def scale_of(parts, entries):
        total = parts[0]
        for p in parts[1:]:
            total = total + p
        return lax.rsqrt(jnp.sum(total, axis=0, keepdims=True).sum(axis=1, keepdims=True) * (1.0 / entries) + grad_epsilon)

    def spans(ref, first, last):
        rows = ref.shape[1]
        while first < last:
            n, inside = first // rows, first % rows
            size = min(rows - inside, last - first)
            yield n, inside, size, first
            first += size

    def squares(ref, first, last, lanes):
        return [
            jnp.sum(jnp.square(ref[n, i : i + s, lanes]), axis=0, keepdims=True)
            for n, i, s, _ in spans(ref, first, last)
        ]

    channels = g_proj_two.shape[0]
    wide = g_merge.shape[0]
    every = slice(0, channels)
    jobs = (
        (g_merge, [(0, wide, 0)]),
        (g_proj_two, [(wide, wide + channels, 0)]),
        (g_qkv_two, [(wide + (n + 1) * channels, wide + (n + 2) * channels, n * channels) for n in range(3)]),
    )
    for out, blocks in jobs:
        parts = [q for first, last, _ in blocks for q in squares(two_ref, first, last, every)]
        scale = scale_of(parts, out.shape[0] * out.shape[1])
        for first, last, lane in blocks:
            for n, i, s, row in spans(two_ref, first, last):
                r = row - first
                out[r : r + s, lane : lane + channels] = (two_ref[n, i : i + s, :] * scale).astype(bf16)
    thin = g_proj_one.shape[0]
    first_half = squares(one_ref, 0, thin, slice(0, 2 * thin))
    second = squares(one_ref, thin, 2 * thin, slice(0, 2 * thin))
    lanes = lax.broadcasted_iota(jnp.int32, (1, 2 * thin), 1)
    qkv_parts = first_half + [jnp.where(lanes < thin, p, 0.0) for p in second]
    proj_parts = [jnp.where(lanes < thin, 0.0, p) for p in second]
    scale_qkv = scale_of(qkv_parts, 3 * thin * thin)
    scale_proj = scale_of(proj_parts, thin * thin)
    for n, i, s, row in spans(one_ref, 0, thin):
        g_qkv_one[row : row + s, 0 : 2 * thin] = (one_ref[n, i : i + s, :] * scale_qkv).astype(bf16)
    for n, i, s, row in spans(one_ref, thin, 2 * thin):
        r = row - thin
        g_qkv_one[r : r + s, 2 * thin : 3 * thin] = (one_ref[n, i : i + s, 0:thin] * scale_qkv).astype(bf16)
        g_proj_one[r : r + s, :] = (one_ref[n, i : i + s, thin : 2 * thin] * scale_proj).astype(bf16)


def shards(
    tokens, cotangent, kinds_one, kinds_two, table_one, table_two, gain_one, gain_merge, gain_two,
    qkv_one, proj_one, merge_weight, qkv_two, proj_two,
):
    c1, c2 = proj_one.shape[0], proj_two.shape[0]
    rows1, cols1 = tokens.shape[1], tokens.shape[2] // c1
    rows2, cols2 = rows1 // 2, cols1 // 2
    nlon, nlat = sizes()
    vmem = pl.BlockSpec(memory_space=pltpu.VMEM)
    stages = place_stages()

    lace1 = lane_rows(rows1, cols1, LEVELS * rows1)
    lace2_pad = rounded_up(LEVELS * rows2, 8)
    lace2 = lane_rows(rows2, cols2, lace2_pad)
    win1, win2 = window_rows(rows1, cols1), window_rows(rows2, cols2)
    group = merge_rows(rows1, cols1)
    ahead = parts_rows(rows1, cols1, True)
    behind = parts_rows(rows1, cols1, False)
    ahead_got = moved(ahead, -HALF_LAT, -HALF_LON, rows1, cols1)
    behind_got = moved(behind, HALF_LAT, HALF_LON, rows1, cols1)
    orders = [
        index_of(win1, lace1),
        index_of(flat(ahead), win1),
        index_of(group, ahead_got),
        index_of(lace2, win2),
        index_of(win2, lace2),
        index_of(flat(behind), group),
        index_of(win1, behind_got),
        index_of(lace1, win1),
    ]
    index = np.full((max(len(o) for o in orders), 128), -1, np.int32)
    for n, order in enumerate(orders):
        index[: len(order), n] = order
    index = jnp.asarray(index)
    sizes_parts = [len(p) for p in ahead]

    lattice = tokens.transpose(1, 0, 2)
    cot = cotangent.transpose(1, 0, 2)
    halos = exchange(*halo_call(lattice, cot, HALF_LON * c1), -1)
    bias_one, bias_two = bias_call(
        kinds_one, kinds_two, table_one.swapaxes(0, 1), table_two.swapaxes(0, 1)
    )

    def part_shapes(dtype=bf16):
        return [jax.ShapeDtypeStruct((n, c1), dtype) for n in sizes_parts]

    count1 = LEVELS * rows1 * cols1
    units1 = count1 // SPOTS
    fwd = pl.pallas_call(
        functools.partial(forward_one_kernel, cols=cols1, columns=(0, 1)),
        name="forward_one",
        in_specs=[vmem] * 9,
        out_specs=[vmem] * 8,
        out_shape=near_out(
            part_shapes()
            + [
                jax.ShapeDtypeStruct((count1, c1), bf16),
                jax.ShapeDtypeStruct((count1, 3 * c1), bf16),
                jax.ShapeDtypeStruct((units1, HEADS1 * SPOTS, 128), bf16),
                jax.ShapeDtypeStruct((count1, c1), bf16),
            ]
        ),
        compiler_params=LIMIT,
        scratch_shapes=[
            pltpu.VMEM((LEVELS * rows1, cols1 * c1), f32),
            pltpu.VMEM((count1, 3 * c1), f32),
            pltpu.VMEM((count1, c1), f32),
        ],
    )(*near_in(lattice, *halos, bias_one, gain_one, qkv_one, proj_one, index))
    parts, kept = fwd[:4], fwd[4:]
    got = exchange(*parts[1:], -1)

    tokens2 = LEVELS * SPOTS
    total_two = 4 * c1 + 4 * c2
    d_block_two = pl.pallas_call(
        functools.partial(cotangent_kernel, thin=c1, cols=cols2, column=4),
        name="cot",
        in_specs=[vmem] * 6,
        out_specs=[vmem] * 2,
        out_shape=[pltpu.VMEM((tokens2, c2), bf16), pltpu.VMEM((tokens2, c2), f32)],
        scratch_shapes=[pltpu.VMEM((lace2_pad, cols2 * c2), f32)],
        compiler_params=LIMIT,
    )(*near_in(cot, *halos, proj_two, index))
    two = pl.pallas_call(
        functools.partial(merge_two_kernel, columns=(2, 5)),
        name="merge_two",
        in_specs=[vmem] * 13,
        out_specs=[vmem] * 7,
        out_shape=near_out(
            [jax.ShapeDtypeStruct((tokens2, c2), bf16)]
            + part_shapes()
            + [jax.ShapeDtypeStruct((total_two // 2, c2), bf16)] * 2
        ),
        compiler_params=LIMIT_TWO,
        scratch_shapes=[
            pltpu.VMEM((LEVELS, HEADS2 * SPOTS, 128), f32),
            pltpu.VMEM((tokens2, 3 * c2), f32),
            pltpu.VMEM((tokens2, c2), f32),
            pltpu.VMEM((tokens2, 3 * c2), f32),
            pltpu.VMEM((total_two, c2), f32),
        ],
    )(*near_in(parts[0], *got, *d_block_two, bias_two, gain_merge, gain_two,
                merge_weight, qkv_two, proj_two, index))
    block_two, d_parts, sums_two = two[0], two[1:5], two[5:]
    d_got = exchange(*d_parts[1:], 1)
    two_parts = [sums_two[0], pair(sums_two[1])]
    for n in range(len(stages)):
        two_parts = moves(sum_split(two_parts, n), n)

    lanes1, lane1 = tokens.shape[2], HALF_LON * c1
    one = pl.pallas_call(
        functools.partial(backward_one_kernel, cols=cols1, columns=(6, 7, 3)),
        name="backward_one",
        in_specs=[vmem] * 13,
        out_specs=[vmem] * 7,
        out_shape=near_out(
            [
                jax.ShapeDtypeStruct((rows2 - HALF_LAT, LEVELS, lanes1 - 2 * lane1), bf16),
                jax.ShapeDtypeStruct((rows1 - HALF_LAT, LEVELS, lanes1 - lane1), bf16),
                *(jax.ShapeDtypeStruct(h.shape, bf16) for h in halos),
            ]
            + [jax.ShapeDtypeStruct((c1, 2 * c1), bf16)] * 2
        ),
        compiler_params=LIMIT,
        scratch_shapes=[
            pltpu.VMEM((LEVELS * rows1, cols1 * c1), f32),
            pltpu.VMEM((count1, 3 * c1), f32),
            pltpu.VMEM((count1, c1), f32),
            pltpu.VMEM((count1, 3 * c1), f32),
            pltpu.VMEM((c1, 4 * c1), f32),
            pltpu.VMEM((lace2_pad, cols2 * c2), f32),
        ],
    )(*near_in(d_parts[0], *d_got, *kept, block_two, gain_one, qkv_one, proj_one, index))
    res_main, d_tok, sums_one = one[0], one[1:5], one[5:]
    one_parts = [sums_one[0], pair(sums_one[1])]
    one_parts = moves(sum_split(one_parts, 0), 0)
    message = message_of(two_parts, one_parts)
    small = one_parts[0].shape[0]
    for n in range(len(stages) - 1, 0, -1):
        message = widen(moves([message] * stages[n][0], n), small)
    own = moves([message] * stages[0][0], 0)
    far = [pair(m) for m in own]
    back = exchange(*d_tok[1:], 1)
    joined = pl.pallas_call(
        join_kernel,
        name="join",
        in_specs=[vmem] * 5,
        out_specs=[vmem] * 2,
        out_shape=[
            jax.ShapeDtypeStruct((rows2, LEVELS, lanes1), bf16),
            jax.ShapeDtypeStruct((rows1, LEVELS, lanes1), bf16),
        ],
        compiler_params=LIMIT,
    )(*near_in(res_main, d_tok[0], *back))
    result, d_tokens = (v.transpose(1, 0, 2) for v in joined)

    near = stages[0][0]
    inner = 1
    for size, _, _ in stages[1:]:
        inner *= size
    grads = pl.pallas_call(
        functools.partial(finish_kernel, stage_sizes=tuple(size for size, _, _ in stages)),
        name="finish",
        in_specs=[vmem] * (2 * near),
        out_specs=[vmem] * 5,
        out_shape=[
            jax.ShapeDtypeStruct(w.shape, bf16) for w in (qkv_one, proj_one, merge_weight, qkv_two, proj_two)
        ],
        scratch_shapes=[
            pltpu.VMEM((2 * near * inner,) + two_parts[0].shape, f32),
            pltpu.VMEM((2 * near,) + one_parts[0].shape, f32),
        ],
        compiler_params=LIMIT,
    )(*near_in(*own, *far))
    return (result, d_tokens, *grads)


def solution(mesh):
    tiled = P(None, "lat", "lon")
    in_specs = (tiled, tiled, P(None, "lat"), P(None, "lat")) + (P(),) * 10
    out_specs = (tiled, tiled, P(), P(), P(), P(), P())

    return jax.shard_map(shards, mesh=mesh, in_specs=in_specs, out_specs=out_specs, check_vma=False)
```
